512 devices in a mesh: seq: 64 (over z_hi, x, y), chan: 8 (over z_lo, core).
Axes of the slice: x: 4, y: 4, z: 16 (z_hi: 4, z_lo: 4; z = z_hi * 4 + z_lo), core: 2. Of those that a mesh axis runs over, the one named last changes fastest.
Arguments:
- query_gate: bfloat16 [4096, 8192], P('chan', 'seq'), may hold values from -6 to 6
- key_gate: bfloat16 [4096, 8192], P('chan', 'seq'), may hold values from -6 to 6
- value_in: bfloat16 [4096, 8192], P('chan', 'seq'), may hold values from -6 to 6
- cotangent: bfloat16 [4096, 8192], P('chan', 'seq'), may hold values from -6 to 6
- long_filter: float32 [4096, 8192], P(('chan', 'seq')), may hold values from -0.0625 to 0.0625
- short_taps: float32 [4096, 3], P('chan'), may hold values from -3 to 3
Outputs:
- query_grad: bfloat16 [4096, 8192], P('chan', 'seq')
- key_grad: bfloat16 [4096, 8192], P('chan', 'seq')
- value_grad: bfloat16 [4096, 8192], P('chan', 'seq')
- filter_grad: float32 [4096, 8192], P(('chan', 'seq'))
- taps_grad: float32 [4096, 3], P('chan')
The draws below stay inside these ranges and needn't reach their ends.
All inputs are finite; a program needn't handle non-finite values.
Results may differ from the reference program's by a relative error of at most 0.0064.
Values may be sent and summed in bfloat16 or wider, within the bound.
A program may use at most 64 MiB of HBM per device.

```python
import math
import jax
import jax.numpy as jnp
from jax import lax

TAPS = 3
LENGTH = 8192
CH = 4096


def shard_levels(rng, extent, pieces, smallest, largest):
    def one(dim, blocks):
        steps = jax.random.uniform(jax.random.fold_in(jax.random.fold_in(rng, 6), dim), (blocks,), jnp.float32, smallest / len(pieces), largest / len(pieces))
        return jnp.repeat(jnp.exp(steps), extent[dim] // blocks).reshape((-1,) + (1,) * (len(extent) - dim - 1))

    factor_of = one(*pieces[0])
    for cut in pieces[1:]:
        factor_of = factor_of * one(*cut)
    return factor_of


def bell_draw(key, shape, deviation, bound, cuts=(), kind=jnp.bfloat16):
    factor_of = shard_levels(key, shape, cuts, -0.22, 0.18) if cuts else 1.0
    values = jax.random.normal(key, shape, jnp.float32) * deviation * factor_of
    return jnp.minimum(jnp.maximum(values, -bound), bound).astype(kind)


def setup_inputs(seed: int = 0) -> dict:
    arg_keys = jax.random.split(jax.random.key(seed), 7)
    query_gate = bell_draw(arg_keys[0], (CH, LENGTH), 1.0, 6.0, ((0, 8), (1, 64)))
    key_gate = bell_draw(arg_keys[1], (CH, LENGTH), 1.0, 6.0, ((0, 8), (1, 64)))
    value_in = bell_draw(arg_keys[2], (CH, LENGTH), 1.0, 6.0, ((0, 8), (1, 64)))
    cotangent = bell_draw(arg_keys[3], (CH, LENGTH), 1.0, 6.0, ((0, 8), (1, 64)))
    long_filter = bell_draw(arg_keys[4], (CH, LENGTH), LENGTH ** -0.5, 0.0625, ((0, 512),), jnp.float32)
    short_taps = bell_draw(arg_keys[5], (CH, TAPS), 0.6, 3.0, ((0, 8),), jnp.float32)
    return {"query_gate": query_gate, "key_gate": key_gate, "value_in": value_in, "cotangent": cotangent, "long_filter": long_filter, "short_taps": short_taps}


def rounded(values):
    return lax.optimization_barrier(values.astype(jnp.bfloat16)).astype(jnp.float32)

def short_filter(stream, weights):
    padded = jnp.pad(stream, ((0, 0), (TAPS - 1, 0)))
    total = jnp.zeros(stream.shape, jnp.float32)
    for lag_index in range(TAPS):
        begin = TAPS - 1 - lag_index
        total = total + weights[:, lag_index:lag_index + 1] * padded[:, begin:begin + LENGTH]
    return (total, padded)

def block_grads(block):
    query_gate, key_gate, value_in, cotangent, long_filter, short_taps = block
    modulus = 2 * LENGTH
    scale = 1.0 / math.sqrt(LENGTH)
    value_f = value_in.astype(jnp.float32)
    key_f = key_gate.astype(jnp.float32)
    cot_f = cotangent.astype(jnp.float32)
    filtered, padded = short_filter(value_f, short_taps)
    mixed = rounded(key_f * filtered)
    conv_grad = rounded(cot_f * query_gate.astype(jnp.float32))
    mixed_spec = jnp.fft.rfft(mixed, n=modulus, axis=1)
    filt_spec = jnp.fft.rfft(long_filter, n=modulus, axis=1)
    grad_spec = jnp.fft.rfft(conv_grad, n=modulus, axis=1)
    conv = rounded(jnp.fft.irfft(mixed_spec * filt_spec, n=modulus, axis=1)[:, :LENGTH])
    mixed_grad = rounded(jnp.fft.irfft(jnp.conj(filt_spec) * grad_spec, n=modulus, axis=1)[:, :LENGTH])
    filter_grad = jnp.fft.irfft(jnp.conj(mixed_spec) * grad_spec, n=modulus, axis=1)[:, :LENGTH] * scale
    query_grad = (cot_f * conv).astype(jnp.bfloat16)
    key_grad = (mixed_grad * filtered).astype(jnp.bfloat16)
    filtered_grad = rounded(mixed_grad * key_f)
    grad_pad = jnp.pad(filtered_grad, ((0, 0), (0, TAPS - 1)))
    value_acc = jnp.zeros(filtered_grad.shape, jnp.float32)
    tap_terms = []
    for lag_index in range(TAPS):
        value_acc = value_acc + short_taps[:, lag_index:lag_index + 1] * grad_pad[:, lag_index:lag_index + LENGTH]
        begin = TAPS - 1 - lag_index
        tap_terms.append(lax.optimization_barrier(jnp.sum(filtered_grad * padded[:, begin:begin + LENGTH], axis=1)))
    value_grad = value_acc.astype(jnp.bfloat16)
    taps_grad = jnp.stack(tap_terms, axis=1) * scale
    return (query_grad, key_grad, value_grad, filter_grad.astype(jnp.float32), taps_grad.astype(jnp.float32))

def reference(query_gate, key_gate, value_in, cotangent, long_filter, short_taps):
    width_block = 128 if CH % 128 == 0 else CH
    block_count = CH // width_block

    def split_rows(array):
        return array.reshape((block_count, width_block) + array.shape[1:])
    blocks = tuple((split_rows(array) for array in (query_gate, key_gate, value_in, cotangent, long_filter, short_taps)))
    results = lax.map(block_grads, blocks)
    return tuple((array.reshape((CH,) + array.shape[2:]) for array in results))
```

```python
import math

import jax
import jax.numpy as jnp
import ml_dtypes
import numpy as np
from jax import lax
from jax.experimental import pallas as pl
from jax.experimental.pallas import tpu as pltpu
from jax.sharding import PartitionSpec as P

TAPS = 3
MESH = pl.DeviceIdType.MESH
BF = jnp.bfloat16
F32 = jnp.float32

S = 64
W = 128
C = 8
N = S * W
PLANE = 16
HI = 4


def halves(table):
    hi = table.astype(ml_dtypes.bfloat16)
    lo = (table - hi.astype(np.float64)).astype(ml_dtypes.bfloat16)
    return hi, lo


def tables():
    quarter = np.arange(S) + 0.25
    rows = 2.0 * np.pi * np.outer(quarter, np.arange(S)) / S
    twist = 2.0 * np.pi * np.outer(quarter, np.arange(W)) / N
    cols = 2.0 * np.pi * np.outer(np.arange(W), np.arange(W)) / W
    a_hi, a_lo = halves(np.concatenate([np.cos(rows), -np.sin(rows)], axis=0))
    b_hi, b_lo = halves(np.concatenate([np.cos(rows).T, -np.sin(rows).T], axis=1) / N)
    fr, fi = np.cos(cols), -np.sin(cols)
    f_hi, f_lo = halves(np.block([[fr, fi], [-fi, fr]]))
    g_hi, g_lo = halves(np.block([[fr, -fi], [fi, fr]]))
    first = np.concatenate([a_hi, a_lo, a_hi, a_lo], axis=1)
    last = np.concatenate([b_hi, b_lo, b_hi], axis=1)
    middle = np.stack([f_hi, f_lo, g_hi, g_lo])
    turn = np.stack([np.cos(twist), -np.sin(twist)]).astype(np.float32)
    return first, middle, last, turn


def split(x):
    hi = x.astype(BF)
    return hi, (x - hi.astype(F32)).astype(BF)


def dot(a, b):
    return jnp.dot(a, b, preferred_element_type=F32)


def wide(table):
    return jnp.concatenate([table] * C, axis=1)


def to_rows(x):
    return jnp.concatenate([x[:, c * W : (c + 1) * W] for c in range(C)], axis=0)


def to_cols(x):
    return jnp.concatenate([x[c * S : (c + 1) * S] for c in range(C)], axis=1)


def forward(stacked, first, middle, turn):
    y = dot(first, stacked)
    yr, yi = y[:S], y[S:]
    tc, ts = wide(turn[0]), wide(turn[1])
    turned = jnp.concatenate([to_rows(yr * tc - yi * ts), to_rows(yr * ts + yi * tc)], axis=1)
    hi, lo = split(turned)
    return dot(hi, middle[0]) + dot(lo, middle[0]) + dot(hi, middle[1])


def inverse(spec_re, spec_im, middle, last, turn):
    hi, lo = split(jnp.concatenate([spec_re, spec_im], axis=1))
    v = dot(hi, middle[2]) + dot(lo, middle[2]) + dot(hi, middle[3])
    vr, vi = to_cols(v[:, :W]), to_cols(v[:, W:])
    tc, ts = wide(turn[0]), wide(turn[1])
    hi, lo = split(jnp.concatenate([vr * tc + vi * ts, vi * tc - vr * ts], axis=0))
    return dot(last[...], jnp.concatenate([hi, hi, lo], axis=0))


def load_signal(ref):
    return jnp.concatenate([ref[pl.ds(c, S, stride=C), :] for c in range(C)], axis=1)


def store_signal(ref, x):
    for c in range(C):
        ref[pl.ds(c, S, stride=C), :] = x[:, c * W : (c + 1) * W]


def row_pick(rows, lanes):
    r = lax.broadcasted_iota(jnp.int32, (8, W), 0)
    l = lax.broadcasted_iota(jnp.int32, (8, W), 1)
    hit = None
    for row, lane in zip(rows, lanes):
        one = (r == row) & (l == lane)
        hit = one if hit is None else hit | one
    return hit.astype(F32)


def pack_pair(x, lanes):
    total = None
    for b in range(4):
        part = lax.dot_general(
            row_pick((2 * b, 2 * b + 1), lanes).astype(BF),
            x[b * W : (b + 1) * W],
            (((1,), (1,)), ((), ())),
            preferred_element_type=F32,
        )
        total = part if total is None else total + part
    return total


def unpack_pair(packed, lanes):
    turned = packed.T.astype(BF)
    return jnp.concatenate(
        [dot(turned, row_pick((2 * b, 2 * b + 1), lanes).astype(BF)) for b in range(4)], axis=0
    )


def main_kernel(
    q_ref, k_ref, v_ref, cot_ref, h_ref, a_ref, first_ref, mid_ref, last_ref, turn_ref,
    qg_ref, kg_ref, vg_ref, fg_ref, tg_ref,
    g_out, g_in, m_out, m_in, b_out, b_in, c_out, c_in,
    vh_out, vh_in, fh_out, fh_in, tp_out, tp_in, tz_out, tz_in,
    rows_ref, filt_ref, low_ref, hs_ref, gs_ref, ms_ref,
    send_sems, recv_sems,
):
    me = lax.axis_index("seq")
    after, before = lax.rem(me + 1, S), lax.rem(me + S - 1, S)
    barrier = pltpu.get_barrier_semaphore()

    def greet(i, carry):
        pl.semaphore_signal(
            barrier, inc=1, device_id={"seq": lax.rem(me + i, S)}, device_id_type=MESH
        )
        return carry

    lax.fori_loop(1, S, greet, 0)

    def remote(src, dst, index, to):
        return pltpu.make_async_remote_copy(
            src_ref=src, dst_ref=dst, send_sem=send_sems.at[index], recv_sem=recv_sems.at[index],
            device_id={"seq": to}, device_id_type=MESH,
        )

    def exchange(out, into, index):
        def one(i, carry):
            to = lax.rem(me + i, S)
            remote(out.at[to], into.at[me], index, to).start()
            return carry

        lax.fori_loop(1, S, one, 0)
        into[me] = out[me]

    def arrived(buffer, sem, count):
        part = buffer.at[pl.ds(0, count)]
        pltpu.make_async_copy(part, part, sem).wait()

    first, turn = first_ref, turn_ref

    cot = cot_ref[...].astype(F32)
    g_out[...] = (cot * q_ref[...].astype(F32)).astype(BF).reshape(S, C, W)
    vh_out[...] = pack_pair(v_ref[...], (W - 2, W - 1))
    for n in range(S):
        rows_ref[n * C : (n + 1) * C, :] = h_ref[:, n * W : (n + 1) * W]
    hi, lo = split(load_signal(rows_ref))
    hs_ref[...] = forward(jnp.concatenate([hi, hi, lo, lo], axis=0), first[...], mid_ref, turn)

    pl.semaphore_wait(barrier, S - 1)

    halo_v = remote(vh_out, vh_in, 0, after)
    halo_v.start()
    exchange(g_out, g_in, 1)

    value = v_ref[...].astype(F32)
    halo_v.wait()
    held = jnp.where(me > 0, vh_in[...], 0.0)
    value_prev = unpack_pair(held, (W - 2, W - 1))
    lane = lax.broadcasted_iota(jnp.int32, (C * S, W), 1)

    def lagged(j):
        if j == 0:
            return value
        return jnp.where(lane < j, pltpu.roll(value_prev, j, 1), pltpu.roll(value, j, 1))

    filtered = a_ref[:, 0:1] * value
    for j in range(1, TAPS):
        filtered = filtered + a_ref[:, j : j + 1] * lagged(j)
    filt_ref[...] = filtered
    m_out[...] = (k_ref[...].astype(F32) * filtered).astype(BF).reshape(S, C, W)
    exchange(m_out, m_in, 2)

    def take(buffer):
        rows_ref[...] = buffer[...].astype(F32).reshape(S * C, W)
        x = load_signal(rows_ref).astype(BF)
        return forward(jnp.concatenate([x, x], axis=0), first[:, : 2 * S], mid_ref, turn)

    def give(buffer, x):
        store_signal(rows_ref, x)
        buffer[...] = rows_ref[...].astype(BF).reshape(S, C, W)

    arrived(g_in, recv_sems.at[1], S - 1)
    grad = take(g_in)
    gs_ref[...] = grad
    hs = hs_ref[...]
    hr, hi_ = hs[:, :W], hs[:, W:]
    gr, gi = grad[:, :W], grad[:, W:]
    give(b_out, inverse(hr * gr + hi_ * gi, hr * gi - hi_ * gr, mid_ref, last_ref, turn))
    exchange(b_out, b_in, 3)

    arrived(m_in, recv_sems.at[2], S - 1)
    mixed = take(m_in)
    ms_ref[...] = mixed
    hs = hs_ref[...]
    hr, hi_ = hs[:, :W], hs[:, W:]
    mr, mi = mixed[:, :W], mixed[:, W:]
    give(c_out, inverse(mr * hr - mi * hi_, mr * hi_ + mi * hr, mid_ref, last_ref, turn))
    exchange(c_out, c_in, 4)

    mixed, grad = ms_ref[...], gs_ref[...]
    mr, mi = mixed[:, :W], mixed[:, W:]
    gr, gi = grad[:, :W], grad[:, W:]
    fg = inverse(mr * gr + mi * gi, mr * gi - mi * gr, mid_ref, last_ref, turn)
    store_signal(rows_ref, fg * (1.0 / math.sqrt(N)))
    for n in range(S):
        fg_ref[:, n * W : (n + 1) * W] = rows_ref[n * C : (n + 1) * C, :]

    arrived(b_in, recv_sems.at[3], S - 1)
    back = b_in[...].astype(F32).reshape(S * C, W)
    kg_ref[...] = (back * filt_ref[...]).astype(BF)
    low_bf = (back * k_ref[...].astype(F32)).astype(BF)
    low_ref[...] = low_bf.astype(F32)
    fh_out[...] = pack_pair(low_bf, (0, 1))
    halo_f = remote(fh_out, fh_in, 5, before)
    halo_f.start()

    low = low_ref[...]
    row8 = lax.broadcasted_iota(jnp.int32, (8, W), 0)
    partial = jnp.zeros((8, 2 * W), F32)
    for j in range(TAPS):
        terms = low * lagged(j)
        t1, rest = split(terms)
        t1f = t1.astype(F32)
        t2, t3 = split(terms - t1f)
        for half in range(2):
            mark = (row8 == 4 * half + j).astype(BF)
            for piece in (t1, t2, t3):
                partial = partial + lax.dot_general(
                    mark, piece[half * 2 * W : (half + 1) * 2 * W], (((1,), (1,)), ((), ())),
                    preferred_element_type=F32,
                )
    tp_out[...] = partial
    place, height = lax.rem(me, PLANE), me // PLANE

    def to_plane(i, carry):
        to = height * PLANE + lax.rem(place + i, PLANE)
        remote(tp_out, tp_in.at[place], 6, to).start()
        return carry

    lax.fori_loop(1, PLANE, to_plane, 0)
    tp_in[place] = tp_out[...]

    halo_f.wait()
    held = jnp.where(me < S - 1, fh_in[...], 0.0)
    low_next = unpack_pair(held, (0, 1))
    value_grad = a_ref[:, 0:1] * low
    for j in range(1, TAPS):
        ahead = jnp.where(lane >= W - j, pltpu.roll(low_next, W - j, 1), pltpu.roll(low, W - j, 1))
        value_grad = value_grad + a_ref[:, j : j + 1] * ahead
    vg_ref[...] = value_grad.astype(BF)

    arrived(tp_in, recv_sems.at[6], PLANE - 1)
    tz_out[...] = jnp.sum(tp_in[...], axis=0)

    def to_heights(i, carry):
        to = lax.rem(height + i, HI) * PLANE + place
        remote(tz_out, tz_in.at[height], 7, to).start()
        return carry

    lax.fori_loop(1, HI, to_heights, 0)
    tz_in[height] = tz_out[...]

    arrived(c_in, recv_sems.at[4], S - 1)
    conv = c_in[...].astype(F32).reshape(S * C, W)
    qg_ref[...] = (cot_ref[...].astype(F32) * conv).astype(BF)

    arrived(tz_in, recv_sems.at[7], HI - 1)
    tg_ref[...] = jnp.sum(tz_in[...], axis=0) * (1.0 / math.sqrt(N))

    arrived(g_out, send_sems.at[1], S - 1)
    arrived(m_out, send_sems.at[2], S - 1)
    arrived(b_out, send_sems.at[3], S - 1)
    arrived(c_out, send_sems.at[4], S - 1)
    arrived(tp_in, send_sems.at[6], PLANE - 1)
    arrived(tz_in, send_sems.at[7], HI - 1)


def write_kernel(q_in, k_in, v_in, f_in, t_in, q_out, k_out, v_out, f_out, t_out):
    q_out[...] = q_in[...]
    k_out[...] = k_in[...]
    v_out[...] = v_in[...]
    f_out[...] = f_in[...]
    turned = t_in[...].T
    t_out[: 2 * W, :] = turned[:, :TAPS]
    t_out[2 * W :, :] = turned[:, 4 : 4 + TAPS]


def on_device(query_gate, key_gate, value_in, cotangent, long_filter, short_taps):
    rows, width = key_gate.shape
    first, middle, last, turn = (jnp.asarray(t) for t in tables())
    vmem = pl.BlockSpec(memory_space=pltpu.VMEM)
    stream = jax.ShapeDtypeStruct((rows, width), BF)
    filt = jax.ShapeDtypeStruct((C, N), F32)
    outs = pl.pallas_call(
        main_kernel,
        out_shape=(stream, stream, stream, filt, jax.ShapeDtypeStruct((8, 2 * W), F32)),
        in_specs=[vmem] * 10,
        out_specs=(vmem,) * 5,
        scratch_shapes=[pltpu.VMEM((S, C, W), BF)] * 8
        + [pltpu.VMEM((8, W), F32)] * 4
        + [
            pltpu.VMEM((8, 2 * W), F32),
            pltpu.VMEM((PLANE, 8, 2 * W), F32),
            pltpu.VMEM((8, 2 * W), F32),
            pltpu.VMEM((HI, 8, 2 * W), F32),
            pltpu.VMEM((S * C, W), F32),
            pltpu.VMEM((S * C, W), F32),
            pltpu.VMEM((S * C, W), F32),
            pltpu.VMEM((S * C, 2 * W), F32),
            pltpu.VMEM((S * C, 2 * W), F32),
            pltpu.VMEM((S * C, 2 * W), F32),
            pltpu.SemaphoreType.DMA((8,)),
            pltpu.SemaphoreType.DMA((8,)),
        ],
        compiler_params=pltpu.CompilerParams(
            collective_id=0, has_side_effects=True, vmem_limit_bytes=48 << 20
        ),
        name="exchange",
    )(query_gate, key_gate, value_in, cotangent, long_filter, short_taps, first, middle, last, turn)
    return pl.pallas_call(
        write_kernel,
        out_shape=(stream, stream, stream, filt, jax.ShapeDtypeStruct((rows, TAPS), F32)),
        in_specs=[vmem] * 5,
        out_specs=(vmem,) * 5,
        name="write",
    )(*outs)


def solution(mesh):
    spec = P("chan", "seq")
    owned = P(("chan", "seq"), None)
    taps = P("chan", None)
    return jax.shard_map(
        on_device,
        mesh=mesh,
        in_specs=(spec, spec, spec, spec, owned, taps),
        out_specs=(spec, spec, spec, owned, taps),
        check_vma=False,
    )
```

```python
import math

import jax
import jax.numpy as jnp
import ml_dtypes
import numpy as np
from jax import lax
from jax.experimental import pallas as pl
from jax.experimental.pallas import tpu as pltpu
from jax.sharding import PartitionSpec as P

TAPS = 3
MESH = pl.DeviceIdType.MESH
BF = jnp.bfloat16
F32 = jnp.float32

S = 64
W = 128
C = 8
N = S * W
PLANE = 16
HI = 4
PARTS = (range(0, 4), range(4, 8))
VMEM_BYTES = 66_900_000


def halves(table):
    hi = table.astype(ml_dtypes.bfloat16)
    lo = (table - hi.astype(np.float64)).astype(ml_dtypes.bfloat16)
    return hi, lo


def tables():
    quarter = np.arange(S) + 0.25
    rows = 2.0 * np.pi * np.outer(quarter, np.arange(S)) / S
    twist = 2.0 * np.pi * np.outer(quarter, np.arange(W)) / N
    cols = 2.0 * np.pi * np.outer(np.arange(W), np.arange(W)) / W
    a_hi, a_lo = halves(np.concatenate([np.cos(rows), -np.sin(rows)], axis=0))
    b_hi, b_lo = halves(np.concatenate([np.cos(rows).T, -np.sin(rows).T], axis=1) / N)
    fr, fi = np.cos(cols), -np.sin(cols)
    f_hi, f_lo = halves(np.block([[fr, fi], [-fi, fr]]))
    g_hi, g_lo = halves(np.block([[fr, -fi], [fi, fr]]))
    first = np.concatenate([a_hi, a_lo, a_hi, a_lo], axis=1)
    last = np.concatenate([b_hi, b_lo, b_hi], axis=1)
    middle = np.stack([f_hi, f_lo, g_hi, g_lo])
    turn = np.stack([np.cos(twist), -np.sin(twist)]).astype(np.float32)
    return first, middle, last, turn


def split(x):
    hi = x.astype(BF)
    return hi, (x - hi.astype(F32)).astype(BF)


def dot(a, b):
    return jnp.dot(a, b, preferred_element_type=F32)


def to_rows(x):
    return jnp.concatenate([x[:, i : i + W] for i in range(0, x.shape[1], W)], axis=0)


def to_cols(x):
    return jnp.concatenate([x[i : i + S] for i in range(0, x.shape[0], S)], axis=1)


def wide(table, like):
    return jnp.concatenate([table] * (like.shape[1] // W), axis=1)


def forward(stacked, first, middle, turn):
    y = dot(first, stacked)
    yr, yi = y[:S], y[S:]
    tc, ts = wide(turn[0], yr), wide(turn[1], yr)
    turned = jnp.concatenate([to_rows(yr * tc - yi * ts), to_rows(yr * ts + yi * tc)], axis=1)
    hi, lo = split(turned)
    return dot(hi, middle[0]) + dot(lo, middle[0]) + dot(hi, middle[1])


def inverse(spec_re, spec_im, middle, last, turn):
    hi, lo = split(jnp.concatenate([spec_re, spec_im], axis=1))
    v = dot(hi, middle[2]) + dot(lo, middle[2]) + dot(hi, middle[3])
    vr, vi = to_cols(v[:, :W]), to_cols(v[:, W:])
    tc, ts = wide(turn[0], vr), wide(turn[1], vr)
    hi, lo = split(jnp.concatenate([vr * tc + vi * ts, vi * tc - vr * ts], axis=0))
    return dot(last[...], jnp.concatenate([hi, hi, lo], axis=0))


def load_signal(ref, channels):
    return jnp.concatenate([ref[pl.ds(c, S, stride=C), :] for c in channels], axis=1)


def store_signal(ref, x, channels):
    for i, c in enumerate(channels):
        ref[pl.ds(c, S, stride=C), :] = x[:, i * W : (i + 1) * W]


def row_pick(rows, lanes):
    r = lax.broadcasted_iota(jnp.int32, (8, W), 0)
    l = lax.broadcasted_iota(jnp.int32, (8, W), 1)
    hit = None
    for row, lane in zip(rows, lanes):
        one = (r == row) & (l == lane)
        hit = one if hit is None else hit | one
    return hit.astype(F32)


def pack_pair(x, lanes):
    total = None
    for b in range(4):
        part = lax.dot_general(
            row_pick((2 * b, 2 * b + 1), lanes).astype(BF),
            x[b * W : (b + 1) * W],
            (((1,), (1,)), ((), ())),
            preferred_element_type=F32,
        )
        total = part if total is None else total + part
    return total


def unpack_pair(packed, lanes):
    turned = packed.T.astype(BF)
    return jnp.concatenate(
        [dot(turned, row_pick((2 * b, 2 * b + 1), lanes).astype(BF)) for b in range(4)], axis=0
    )


def main_kernel(
    q_hbm, k_hbm, v_hbm, cot_hbm, h_hbm, a_hbm, first_hbm, mid_hbm, last_hbm, turn_hbm,
    qg_hbm, kg_hbm, vg_hbm, fg_hbm, tg_hbm,
    g_out, g_in, m_out, m_in, b_out, b_in, c_out, c_in,
    vh_out, vh_in, fh_out, fh_in, tp_out, tp_in, tz_out, tz_in,
    rows_ref, filt_ref, low_ref, hs_ref, gs_ref, ms_ref,
    q_ref, k_ref, v_ref, cot_ref, h_ref, a_ref, first_ref, mid_ref, last_ref, turn_ref,
    qg_ref, kg_ref, vg_ref, fg_ref, tg_ref,
    send_sems, recv_sems, load_sems, store_sems,
):
    loads = [
        pltpu.make_async_copy(src, dst, load_sems.at[i])
        for i, (src, dst) in enumerate((
            (h_hbm, h_ref), (first_hbm, first_ref), (turn_hbm, turn_ref), (mid_hbm, mid_ref),
            (cot_hbm, cot_ref), (q_hbm, q_ref), (v_hbm, v_ref), (a_hbm, a_ref),
            (k_hbm, k_ref), (last_hbm, last_ref),
        ))
    ]
    stores = [
        pltpu.make_async_copy(src, dst, store_sems.at[i])
        for i, (src, dst) in enumerate((
            (qg_ref, qg_hbm), (kg_ref, kg_hbm), (vg_ref, vg_hbm), (fg_ref, fg_hbm), (tg_ref, tg_hbm),
        ))
    ]
    me = lax.axis_index("seq")
    after, before = lax.rem(me + 1, S), lax.rem(me + S - 1, S)
    barrier = pltpu.get_barrier_semaphore()

    place, height = lax.rem(me, PLANE), me // PLANE

    def to_all(act):
        heights = [lax.rem(height + h, HI) * PLANE for h in (2, 1, 3, 0)]
        for base in heights[:3]:
            act(base + place)

        def one(i, carry):
            at = lax.rem(place + i, PLANE)
            for base in heights:
                act(base + at)
            return carry

        lax.fori_loop(1, PLANE, one, 0)

    to_all(
        lambda to: pl.semaphore_signal(barrier, inc=1, device_id={"seq": to}, device_id_type=MESH)
    )
    for load in loads:
        load.start()

    def remote(src, dst, index, to):
        return pltpu.make_async_remote_copy(
            src_ref=src, dst_ref=dst, send_sem=send_sems.at[index], recv_sem=recv_sems.at[index],
            device_id={"seq": to}, device_id_type=MESH,
        )

    def exchange(out, into, index, channels=range(C)):
        part = pl.ds(channels[0], len(channels))
        to_all(lambda to: remote(out.at[to, part], into.at[me, part], index, to).start())
        into[me, part] = out[me, part]

    def arrived(buffer, sem, count):
        part = buffer.at[pl.ds(0, count)]
        pltpu.make_async_copy(part, part, sem).wait()

    def exchanged(buffer, sem, channels=range(C)):
        part = buffer.at[pl.ds(0, S - 1), pl.ds(channels[0], len(channels))]
        pltpu.make_async_copy(part, part, sem).wait()

    first, turn = first_ref, turn_ref
    tiles_ref = rows_ref.reshape(S, C, W)

    with jax.named_scope("local"):
        for load in loads:
            load.wait()
        cot = cot_ref[...].astype(F32)
        g_out[...] = (cot * q_ref[...].astype(F32)).astype(BF).reshape(S, C, W)
        vh_out[...] = pack_pair(v_ref[...], (W - 2, W - 1))
        for n in range(S):
            rows_ref[n * C : (n + 1) * C, :] = h_ref[:, n * W : (n + 1) * W]
        hi, lo = split(load_signal(rows_ref, range(C)))
        hs_ref[...] = forward(jnp.concatenate([hi, hi, lo, lo], axis=0), first[...], mid_ref, turn)

    with jax.named_scope("wait_barrier"):
        pl.semaphore_wait(barrier, S - 1)

    halo_v = remote(vh_out, vh_in, 0, after)
    halo_v.start()
    with jax.named_scope("send_g"):
        for index, channels in zip((1, 8), PARTS):
            exchange(g_out, g_in, index, channels)

    value = v_ref[...].astype(F32)
    a_all = a_ref[...]
    taps = jnp.concatenate(
        [
            jnp.concatenate([a_all[:, b * W : (b + 1) * W], jnp.zeros((8 - TAPS, W), F32)], axis=0).T
            for b in range(4)
        ],
        axis=0,
    )
    with jax.named_scope("wait_halo_v"):
        halo_v.wait()
    held = jnp.where(me > 0, vh_in[...], 0.0)
    value_prev = unpack_pair(held, (W - 2, W - 1))
    lane = lax.broadcasted_iota(jnp.int32, (C * S, W), 1)

    def lagged(j):
        if j == 0:
            return value
        return jnp.where(lane < j, pltpu.roll(value_prev, j, 1), pltpu.roll(value, j, 1))

    filtered = taps[:, 0:1] * value
    for j in range(1, TAPS):
        filtered = filtered + taps[:, j : j + 1] * lagged(j)
    filt_ref[...] = filtered
    m_out[...] = (k_ref[...].astype(F32) * filtered).astype(BF).reshape(S, C, W)
    with jax.named_scope("send_m"):
        exchange(m_out, m_in, 2)

    def take(buffer, channels):
        part = pl.ds(channels[0], len(channels))
        tiles_ref[:, part, :] = buffer[:, part, :].astype(F32)
        x = load_signal(rows_ref, channels).astype(BF)
        return forward(jnp.concatenate([x, x], axis=0), first[:, : 2 * S], mid_ref, turn)

    def give(buffer, x, channels):
        part = pl.ds(channels[0], len(channels))
        store_signal(rows_ref, x, channels)
        buffer[:, part, :] = tiles_ref[:, part, :].astype(BF)

    for index, channels in zip((1, 8), PARTS):
        with jax.named_scope("wait_g"):
            exchanged(g_in, recv_sems.at[index], channels)
        grad = take(g_in, channels)
        mine = pl.ds(channels[0] * S, len(channels) * S)
        gs_ref[mine, :] = grad
        hs = hs_ref[mine, :]
        hr, hi_ = hs[:, :W], hs[:, W:]
        gr, gi = grad[:, :W], grad[:, W:]
        back = inverse(hr * gr + hi_ * gi, hr * gi - hi_ * gr, mid_ref, last_ref, turn)
        give(b_out, back, channels)
        with jax.named_scope("send_b"):
            exchange(b_out, b_in, index + 2, channels)

    with jax.named_scope("wait_m"):
        exchanged(m_in, recv_sems.at[2])
    mixed = take(m_in, range(C))
    ms_ref[...] = mixed
    hs = hs_ref[...]
    hr, hi_ = hs[:, :W], hs[:, W:]
    mr, mi = mixed[:, :W], mixed[:, W:]
    conv = inverse(mr * hr - mi * hi_, mr * hi_ + mi * hr, mid_ref, last_ref, turn)
    give(c_out, conv, range(C))
    with jax.named_scope("send_c"):
        exchange(c_out, c_in, 4)

    mixed, grad = ms_ref[...], gs_ref[...]
    mr, mi = mixed[:, :W], mixed[:, W:]
    gr, gi = grad[:, :W], grad[:, W:]
    fg = inverse(mr * gr + mi * gi, mr * gi - mi * gr, mid_ref, last_ref, turn)
    store_signal(rows_ref, fg * (1.0 / math.sqrt(N)), range(C))
    for n in range(S):
        fg_ref[:, n * W : (n + 1) * W] = rows_ref[n * C : (n + 1) * C, :]
    stores[3].start()

    with jax.named_scope("wait_b"):
        for index, channels in zip((3, 10), PARTS):
            exchanged(b_in, recv_sems.at[index], channels)
    back = b_in[...].astype(F32).reshape(S * C, W)
    low_bf = (back * k_ref[...].astype(F32)).astype(BF)
    low_ref[...] = low_bf.astype(F32)
    fh_out[...] = pack_pair(low_bf, (0, 1))
    halo_f = remote(fh_out, fh_in, 5, before)
    halo_f.start()

    low = low_ref[...]
    row8 = lax.broadcasted_iota(jnp.int32, (8, W), 0)
    partial = jnp.zeros((8, 2 * W), F32)
    for j in range(TAPS):
        pieces = split(low * lagged(j))
        for half in range(2):
            mark = (row8 == 4 * half + j).astype(BF)
            for piece in pieces:
                partial = partial + lax.dot_general(
                    mark, piece[half * 2 * W : (half + 1) * 2 * W], (((1,), (1,)), ((), ())),
                    preferred_element_type=F32,
                )
    tp_out[...] = partial
    def to_plane(i, carry):
        to = height * PLANE + lax.rem(place + i, PLANE)
        remote(tp_out, tp_in.at[place], 6, to).start()
        return carry

    with jax.named_scope("send_tp"):
        lax.fori_loop(1, PLANE, to_plane, 0)
    tp_in[place] = tp_out[...]

    kg_ref[...] = (b_in[...].astype(F32).reshape(S * C, W) * filt_ref[...]).astype(BF)
    stores[1].start()

    with jax.named_scope("wait_tp"):
        arrived(tp_in, recv_sems.at[6], PLANE - 1)
    tz_out[...] = jnp.sum(tp_in[...], axis=0)

    def to_heights(i, carry):
        to = lax.rem(height + i, HI) * PLANE + place
        remote(tz_out, tz_in.at[height], 7, to).start()
        return carry

    lax.fori_loop(1, HI, to_heights, 0)
    tz_in[height] = tz_out[...]

    with jax.named_scope("wait_halo_f"):
        halo_f.wait()
    held = jnp.where(me < S - 1, fh_in[...], 0.0)
    low_next = unpack_pair(held, (0, 1))
    value_grad = taps[:, 0:1] * low
    for j in range(1, TAPS):
        ahead = jnp.where(lane >= W - j, pltpu.roll(low_next, W - j, 1), pltpu.roll(low, W - j, 1))
        value_grad = value_grad + taps[:, j : j + 1] * ahead
    vg_ref[...] = value_grad.astype(BF)
    stores[2].start()

    with jax.named_scope("wait_c"):
        exchanged(c_in, recv_sems.at[4])
    conv = c_in[...].astype(F32).reshape(S * C, W)
    qg_ref[...] = (cot_ref[...].astype(F32) * conv).astype(BF)
    stores[0].start()

    with jax.named_scope("wait_tz"):
        arrived(tz_in, recv_sems.at[7], HI - 1)
    sums = jnp.sum(tz_in[...], axis=0) * (1.0 / math.sqrt(N))
    tg_ref[:, : 2 * W] = sums[:TAPS]
    tg_ref[:, 2 * W :] = sums[4 : 4 + TAPS]
    stores[4].start()

    for index, channels in zip((1, 8), PARTS):
        exchanged(g_out, send_sems.at[index], channels)
        exchanged(b_out, send_sems.at[index + 2], channels)
    exchanged(m_out, send_sems.at[2])
    exchanged(c_out, send_sems.at[4])
    arrived(tp_in, send_sems.at[6], PLANE - 1)
    arrived(tz_in, send_sems.at[7], HI - 1)
    for store in stores:
        store.wait()


def write_kernel(*refs):
    ins, outs, held, sems, more = refs[:5], refs[5:10], refs[10:15], refs[15], refs[16]
    loads = [
        pltpu.make_async_copy(src, dst, sems.at[i]) for i, (src, dst) in enumerate(zip(ins, held))
    ]
    stores = [
        pltpu.make_async_copy(src, dst, more.at[i]) for i, (src, dst) in enumerate(zip(held, outs))
    ]
    for load in loads:
        load.start()
    for load, store in zip(loads, stores):
        load.wait()
        store.start()
    for store in stores:
        store.wait()


def on_device(query_gate, key_gate, value_in, cotangent, long_filter, short_taps):
    rows, width = key_gate.shape
    first, middle, last, turn = (jnp.asarray(t) for t in tables())
    hbm = pl.BlockSpec(memory_space=pltpu.HBM)
    stream = jax.ShapeDtypeStruct((rows, width), BF)
    filt = jax.ShapeDtypeStruct((C, N), F32)
    shapes = (stream, stream, stream, filt, jax.ShapeDtypeStruct((TAPS, rows), F32))
    operands = (query_gate, key_gate, value_in, cotangent, long_filter, short_taps.T, first, middle, last, turn)
    outs = pl.pallas_call(
        main_kernel,
        out_shape=shapes,
        in_specs=[hbm] * 10,
        out_specs=(hbm,) * 5,
        scratch_shapes=[pltpu.VMEM((S, C, W), BF)] * 8
        + [pltpu.VMEM((8, W), F32)] * 4
        + [
            pltpu.VMEM((8, 2 * W), F32),
            pltpu.VMEM((PLANE, 8, 2 * W), F32),
            pltpu.VMEM((8, 2 * W), F32),
            pltpu.VMEM((HI, 8, 2 * W), F32),
            pltpu.VMEM((S * C, W), F32),
            pltpu.VMEM((S * C, W), F32),
            pltpu.VMEM((S * C, W), F32),
            pltpu.VMEM((S * C, 2 * W), F32),
            pltpu.VMEM((S * C, 2 * W), F32),
            pltpu.VMEM((S * C, 2 * W), F32),
        ]
        + [pltpu.VMEM(x.shape, x.dtype) for x in (*operands, *shapes)]
        + [
            pltpu.SemaphoreType.DMA((11,)),
            pltpu.SemaphoreType.DMA((11,)),
            pltpu.SemaphoreType.DMA((len(operands),)),
            pltpu.SemaphoreType.DMA((len(shapes),)),
        ],
        compiler_params=pltpu.CompilerParams(
            collective_id=0, has_side_effects=True, vmem_limit_bytes=VMEM_BYTES
        ),
        name="exchange",
    )(*operands)
    *streams, tap_sums = pl.pallas_call(
        write_kernel,
        out_shape=shapes,
        in_specs=[hbm] * 5,
        out_specs=(hbm,) * 5,
        scratch_shapes=[pltpu.VMEM(x.shape, x.dtype) for x in shapes]
        + [pltpu.SemaphoreType.DMA((5,)), pltpu.SemaphoreType.DMA((5,))],
        compiler_params=pltpu.CompilerParams(vmem_limit_bytes=VMEM_BYTES),
        name="write",
    )(*outs)
    return (*streams, tap_sums.T)


def solution(mesh):
    spec = P("chan", "seq")
    owned = P(("chan", "seq"), None)
    taps = P("chan", None)
    return jax.shard_map(
        on_device,
        mesh=mesh,
        in_specs=(spec, spec, spec, spec, owned, taps),
        out_specs=(spec, spec, spec, owned, taps),
        check_vma=False,
    )
```

```python
import math

import jax
import jax.numpy as jnp
import ml_dtypes
import numpy as np
from jax import lax
from jax.experimental import pallas as pl
from jax.experimental.pallas import tpu as pltpu
from jax.sharding import PartitionSpec as P

TAPS = 3
MESH = pl.DeviceIdType.MESH
BF = jnp.bfloat16
F32 = jnp.float32

S = 64
W = 128
C = 8
N = S * W
PLANE = 16
HI = 4
PARTS = (range(0, 4), range(4, 6), range(6, 8))
WHOLE = range(C)
PLANE_SUM, HEIGHT_SUM, VALUE_HALO, GRAD_HALO, MIXED, CONV, GRAD = range(7)
BACK = GRAD + len(PARTS)
SEMAPHORES = BACK + len(PARTS)
VMEM_BYTES = 55_820_000
WRITE_BYTES = 4_000_000


def halves(table):
    hi = table.astype(ml_dtypes.bfloat16)
    lo = (table - hi.astype(np.float64)).astype(ml_dtypes.bfloat16)
    return hi, lo


def tables():
    quarter = np.arange(S) + 0.25
    rows = 2.0 * np.pi * np.outer(quarter, np.arange(S)) / S
    twist = 2.0 * np.pi * np.outer(quarter, np.arange(W)) / N
    cols = 2.0 * np.pi * np.outer(np.arange(W), np.arange(W)) / W
    a_hi, a_lo = halves(np.concatenate([np.cos(rows), -np.sin(rows)], axis=0))
    b_hi, b_lo = halves(np.concatenate([np.cos(rows).T, -np.sin(rows).T], axis=1) / N)
    fr, fi = np.cos(cols), -np.sin(cols)
    f_hi, f_lo = halves(np.block([[fr, fi], [-fi, fr]]))
    g_hi, g_lo = halves(np.block([[fr, -fi], [fi, fr]]))
    turn = np.concatenate([np.cos(twist), -np.sin(twist)], axis=1)
    turn_hi, turn_lo = halves(turn)
    turn_rest = (turn - turn_hi.astype(np.float64) - turn_lo.astype(np.float64)).astype(ml_dtypes.bfloat16)
    return np.concatenate(
        [
            f_hi, f_lo, g_hi, g_lo,
            np.concatenate([a_hi, a_lo, a_hi, a_lo], axis=1),
            np.concatenate([b_hi, b_lo], axis=1), turn_hi, turn_lo, turn_rest,
        ],
        axis=0,
    )


def split(x):
    hi = x.astype(BF)
    return hi, (x - hi.astype(F32)).astype(BF)


def dot(a, b):
    return jnp.dot(a, b, preferred_element_type=F32)


def to_rows(x):
    return jnp.concatenate([x[:, i : i + W] for i in range(0, x.shape[1], W)], axis=0)


def to_cols(x):
    return jnp.concatenate([x[i : i + S] for i in range(0, x.shape[0], S)], axis=1)


def wide(table, like):
    return jnp.concatenate([table] * (like.shape[1] // W), axis=1)


def forward(stacked, first, middle, turn):
    y = dot(first, stacked)
    yr, yi = y[:S], y[S:]
    tc, ts = wide(turn[0], yr), wide(turn[1], yr)
    turned = jnp.concatenate([to_rows(yr * tc - yi * ts), to_rows(yr * ts + yi * tc)], axis=1)
    hi, lo = split(turned)
    return dot(hi, middle(0)) + dot(lo, middle(0)) + dot(hi, middle(1))


def inverse(spec_re, spec_im, middle, last, turn):
    hi, lo = split(jnp.concatenate([spec_re, spec_im], axis=1))
    v = dot(hi, middle(2)) + dot(lo, middle(2)) + dot(hi, middle(3))
    vr, vi = to_cols(v[:, :W]), to_cols(v[:, W:])
    tc, ts = wide(turn[0], vr), wide(turn[1], vr)
    hi, lo = split(jnp.concatenate([vr * tc + vi * ts, vi * tc - vr * ts], axis=0))
    return dot(last(), jnp.concatenate([hi, hi, lo], axis=0))


def load_signal(ref, channels):
    return jnp.concatenate([ref[pl.ds(c, S, stride=C), :] for c in channels], axis=1)


def store_signal(ref, x, channels):
    for i, c in enumerate(channels):
        ref[pl.ds(c, S, stride=C), :] = x[:, i * W : (i + 1) * W]


def row_pick(rows, lanes):
    r = lax.broadcasted_iota(jnp.int32, (8, W), 0)
    l = lax.broadcasted_iota(jnp.int32, (8, W), 1)
    hit = None
    for row, lane in zip(rows, lanes):
        one = (r == row) & (l == lane)
        hit = one if hit is None else hit | one
    return hit.astype(F32)


def pack_pair(x, lanes):
    total = None
    for b in range(4):
        part = lax.dot_general(
            row_pick((2 * b, 2 * b + 1), lanes).astype(BF),
            x[b * W : (b + 1) * W],
            (((1,), (1,)), ((), ())),
            preferred_element_type=F32,
        )
        total = part if total is None else total + part
    return total


def unpack_pair(packed, lanes):
    turned = packed.T.astype(BF)
    return jnp.concatenate(
        [dot(turned, row_pick((2 * b, 2 * b + 1), lanes).astype(BF)) for b in range(4)], axis=0
    )


def main_kernel(
    q_hbm, k_hbm, v_hbm, cot_hbm, h_hbm, a_hbm, table_hbm,
    qg_ref, kg_ref, vg_ref, fg_ref, fg_more, tg_ref,
    g_out, g_in, m_out, m_in, b_out, b_in, c_out, c_in,
    vh_out, vh_in, fh_out, fh_in, tp_out, tp_in, tz_out, tz_in,
    rows_ref, filt_ref, low_ref, lag_ref, hs_ref, gs_ref, ms_ref,
    q_ref, k_ref, v_ref, cot_ref, h_ref, a_ref, table_ref, turn_ref,
    send_sems, recv_sems, load_sems,
):
    loads = [
        pltpu.make_async_copy(src, dst, load_sems.at[i])
        for i, (src, dst) in enumerate((
            (h_hbm, h_ref), (table_hbm, table_ref), (cot_hbm, cot_ref), (q_hbm, q_ref),
            (v_hbm, v_ref), (a_hbm, a_ref), (k_hbm, k_ref),
        ))
    ]
    me = lax.axis_index("seq")
    after, before = lax.rem(me + 1, S), lax.rem(me + S - 1, S)
    barrier = pltpu.get_barrier_semaphore()

    place, height = lax.rem(me, PLANE), me // PLANE

    def to_all(act):
        heights = [lax.rem(height + h, HI) * PLANE for h in (2, 1, 3, 0)]
        for base in heights[:3]:
            act(base + place)

        def one(i, carry):
            at = lax.rem(place + i, PLANE)
            for base in heights:
                act(base + at)
            return carry

        lax.fori_loop(1, PLANE, one, 0)

    to_all(
        lambda to: pl.semaphore_signal(barrier, inc=1, device_id={"seq": to}, device_id_type=MESH)
    )
    for load in loads:
        load.start()

    def remote(src, dst, index, to):
        return pltpu.make_async_remote_copy(
            src_ref=src, dst_ref=dst, send_sem=send_sems.at[index], recv_sem=recv_sems.at[index],
            device_id={"seq": to}, device_id_type=MESH,
        )

    def exchange(out, into, index, channels):
        part = pl.ds(channels[0], len(channels))
        to_all(lambda to: remote(out.at[to, part], into.at[me, part], index, to).start())
        into[me, part] = out[me, part]

    def arrived(buffer, sem, count):
        part = buffer.at[pl.ds(0, count)]
        pltpu.make_async_copy(part, part, sem).wait()

    def exchanged(buffer, sem, channels):
        part = buffer.at[pl.ds(0, S - 1), pl.ds(channels[0], len(channels))]
        pltpu.make_async_copy(part, part, sem).wait()

    first = table_ref.at[pl.ds(1024, 2 * S)]
    turn = turn_ref

    def mid_ref(i):
        return table_ref[256 * i : 256 * (i + 1), :]

    def last_ref():
        back = table_ref[1152 : 1152 + S, :]
        return jnp.concatenate([back, back[:, : 2 * S]], axis=1)

    tiles_ref = rows_ref.reshape(S, C, W)

    with jax.named_scope("local"):
        for load in loads:
            load.wait()
        pieces = [table_ref[1216 + i * S : 1216 + (i + 1) * S, :].astype(F32) for i in range(3)]
        turned = pieces[0] + pieces[1] + pieces[2]
        turn_ref[0] = turned[:, :W]
        turn_ref[1] = turned[:, W:]
        cot = cot_ref[...].astype(F32)
        g_out[...] = (cot * q_ref[...].astype(F32)).astype(BF).reshape(S, C, W)
        vh_out[...] = pack_pair(v_ref[...], (W - 2, W - 1))
        for n in range(S):
            rows_ref[n * C : (n + 1) * C, :] = h_ref[:, n * W : (n + 1) * W]
        hi, lo = split(load_signal(rows_ref, range(C)))
        hs_ref[...] = forward(jnp.concatenate([hi, hi, lo, lo], axis=0), first[...], mid_ref, turn)

    with jax.named_scope("wait_barrier"):
        pl.semaphore_wait(barrier, S - 1)

    halo_v = remote(vh_out, vh_in, VALUE_HALO, after)
    halo_v.start()
    with jax.named_scope("send_g"):
        for i, channels in enumerate(PARTS):
            exchange(g_out, g_in, GRAD + i, channels)

    value = v_ref[...].astype(F32)
    a_all = a_ref[...]
    taps = jnp.concatenate(
        [
            jnp.concatenate([a_all[:, b * W : (b + 1) * W], jnp.zeros((8 - TAPS, W), F32)], axis=0).T
            for b in range(4)
        ],
        axis=0,
    )
    with jax.named_scope("wait_halo_v"):
        halo_v.wait()
    held = jnp.where(me > 0, vh_in[...], 0.0)
    value_prev = unpack_pair(held, (W - 2, W - 1))
    lane = lax.broadcasted_iota(jnp.int32, (C * S, W), 1)

    def lagged(j):
        return jnp.where(lane < j, pltpu.roll(value_prev, j, 1), pltpu.roll(value, j, 1))

    filtered = taps[:, 0:1] * value
    lag_ref[0] = value
    for j in range(1, TAPS):
        lag_ref[j] = lagged(j)
        filtered = filtered + taps[:, j : j + 1] * lag_ref[j]
    filt_ref[...] = filtered
    m_out[...] = (k_ref[...].astype(F32) * filtered).astype(BF).reshape(S, C, W)
    with jax.named_scope("send_m"):
        exchange(m_out, m_in, MIXED, WHOLE)

    def take(buffer, channels):
        part = pl.ds(channels[0], len(channels))
        tiles_ref[:, part, :] = buffer[:, part, :].astype(F32)
        x = load_signal(rows_ref, channels).astype(BF)
        return forward(jnp.concatenate([x, x], axis=0), first[:, : 2 * S], mid_ref, turn)

    def give(buffer, x, channels):
        part = pl.ds(channels[0], len(channels))
        store_signal(rows_ref, x, channels)
        buffer[:, part, :] = tiles_ref[:, part, :].astype(BF)

    for i, channels in enumerate(PARTS):
        with jax.named_scope("wait_g"):
            exchanged(g_in, recv_sems.at[GRAD + i], channels)
        grad = take(g_in, channels)
        mine = pl.ds(channels[0] * S, len(channels) * S)
        gs_ref[mine, :] = grad
        hs = hs_ref[mine, :]
        hr, hi_ = hs[:, :W], hs[:, W:]
        gr, gi = grad[:, :W], grad[:, W:]
        back = inverse(hr * gr + hi_ * gi, hr * gi - hi_ * gr, mid_ref, last_ref, turn)
        give(b_out, back, channels)
        with jax.named_scope("send_b"):
            exchange(b_out, b_in, BACK + i, channels)

    with jax.named_scope("wait_m"):
        exchanged(m_in, recv_sems.at[MIXED], WHOLE)
    mixed = take(m_in, WHOLE)
    ms_ref[...] = mixed
    hs = hs_ref[...]
    hr, hi_ = hs[:, :W], hs[:, W:]
    mr, mi = mixed[:, :W], mixed[:, W:]
    conv = inverse(mr * hr - mi * hi_, mr * hi_ + mi * hr, mid_ref, last_ref, turn)
    give(c_out, conv, WHOLE)
    with jax.named_scope("send_c"):
        exchange(c_out, c_in, CONV, WHOLE)

    mixed, grad = ms_ref[...], gs_ref[...]
    mr, mi = mixed[:, :W], mixed[:, W:]
    gr, gi = grad[:, :W], grad[:, W:]
    fg = inverse(mr * gr + mi * gi, mr * gi - mi * gr, mid_ref, last_ref, turn)
    store_signal(rows_ref, fg * (1.0 / math.sqrt(N)), range(C))
    for n in range(S):
        part, at = (fg_ref, n * W) if n < S // 2 else (fg_more, (n - S // 2) * W)
        part[:, at : at + W] = rows_ref[n * C : (n + 1) * C, :]

    with jax.named_scope("wait_b"):
        for i, channels in enumerate(PARTS):
            exchanged(b_in, recv_sems.at[BACK + i], channels)
    back = b_in[...].astype(F32).reshape(S * C, W)
    low_bf = (back * k_ref[...].astype(F32)).astype(BF)
    low_ref[...] = low_bf.astype(F32)
    low = low_ref[...]
    row8 = lax.broadcasted_iota(jnp.int32, (8, W), 0)
    partial = jnp.zeros((8, 2 * W), F32)
    for j in range(TAPS):
        pieces = split(low * lag_ref[j])
        for half in range(2):
            mark = (row8 == 4 * half + j).astype(BF)
            for piece in pieces:
                partial = partial + lax.dot_general(
                    mark, piece[half * 2 * W : (half + 1) * 2 * W], (((1,), (1,)), ((), ())),
                    preferred_element_type=F32,
                )
    tp_out[...] = partial
    def to_plane(i, carry):
        to = height * PLANE + lax.rem(place + i, PLANE)
        remote(tp_out, tp_in.at[place], PLANE_SUM, to).start()
        return carry

    with jax.named_scope("send_tp"):
        lax.fori_loop(1, PLANE, to_plane, 0)
    tp_in[place] = tp_out[...]

    fh_out[...] = pack_pair(low_bf, (0, 1))
    halo_f = remote(fh_out, fh_in, GRAD_HALO, before)
    halo_f.start()
    kg_ref[...] = (b_in[...].astype(F32).reshape(S * C, W) * filt_ref[...]).astype(BF)

    with jax.named_scope("wait_tp"):
        arrived(tp_in, recv_sems.at[PLANE_SUM], PLANE - 1)
    tz_out[...] = jnp.sum(tp_in[...], axis=0)

    def to_heights(i, carry):
        to = lax.rem(height + i, HI) * PLANE + place
        remote(tz_out, tz_in.at[height], HEIGHT_SUM, to).start()
        return carry

    lax.fori_loop(1, HI, to_heights, 0)
    tz_in[height] = tz_out[...]

    with jax.named_scope("wait_halo_f"):
        halo_f.wait()
    held = jnp.where(me < S - 1, fh_in[...], 0.0)
    low_next = unpack_pair(held, (0, 1))
    value_grad = taps[:, 0:1] * low
    for j in range(1, TAPS):
        ahead = jnp.where(lane >= W - j, pltpu.roll(low_next, W - j, 1), pltpu.roll(low, W - j, 1))
        value_grad = value_grad + taps[:, j : j + 1] * ahead
    vg_ref[...] = value_grad.astype(BF)

    with jax.named_scope("wait_c"):
        exchanged(c_in, recv_sems.at[CONV], WHOLE)
    conv = c_in[...].astype(F32).reshape(S * C, W)
    qg_ref[...] = (cot_ref[...].astype(F32) * conv).astype(BF)

    with jax.named_scope("wait_tz"):
        arrived(tz_in, recv_sems.at[HEIGHT_SUM], HI - 1)
    sums = jnp.sum(tz_in[...], axis=0) * (1.0 / math.sqrt(N))
    tg_ref[:, : 2 * W] = sums[:TAPS]
    tg_ref[:, 2 * W :] = sums[4 : 4 + TAPS]

    for i, channels in enumerate(PARTS):
        exchanged(g_out, send_sems.at[GRAD + i], channels)
        exchanged(b_out, send_sems.at[BACK + i], channels)
    exchanged(m_out, send_sems.at[MIXED], WHOLE)
    exchanged(c_out, send_sems.at[CONV], WHOLE)
    arrived(tp_in, send_sems.at[PLANE_SUM], PLANE - 1)
    arrived(tz_in, send_sems.at[HEIGHT_SUM], HI - 1)


def write_kernel(qg, kg, vg, fg, fg_more, tg, qg_out, kg_out, vg_out, fg_out, tg_out, sems):
    pairs = (
        (qg, qg_out), (kg, kg_out), (vg, vg_out), (tg, tg_out),
        (fg, fg_out.at[:, pl.ds(0, N // 2)]), (fg_more, fg_out.at[:, pl.ds(N // 2, N // 2)]),
    )
    copies = [pltpu.make_async_copy(src, dst, sems.at[i]) for i, (src, dst) in enumerate(pairs)]
    for copy in copies:
        copy.start()
    for copy in copies:
        copy.wait()


def on_device(query_gate, key_gate, value_in, cotangent, long_filter, short_taps):
    rows, width = key_gate.shape
    table = jnp.asarray(tables())
    hbm = pl.BlockSpec(memory_space=pltpu.HBM)
    vmem = pl.BlockSpec(memory_space=pltpu.VMEM)
    stream = jax.ShapeDtypeStruct((rows, width), BF)
    filt = jax.ShapeDtypeStruct((C, N), F32)
    half = jax.ShapeDtypeStruct((C, N // 2), F32)
    tap_rows = jax.ShapeDtypeStruct((TAPS, rows), F32)
    operands = (query_gate, key_gate, value_in, cotangent, long_filter, short_taps.T, table)
    outs = pl.pallas_call(
        main_kernel,
        out_shape=(stream, stream, stream, half, half, tap_rows),
        in_specs=[hbm] * len(operands),
        out_specs=(vmem,) * 6,
        scratch_shapes=[pltpu.VMEM((S, C, W), BF)] * 8
        + [pltpu.VMEM((8, W), F32)] * 4
        + [
            pltpu.VMEM((8, 2 * W), F32),
            pltpu.VMEM((PLANE, 8, 2 * W), F32),
            pltpu.VMEM((8, 2 * W), F32),
            pltpu.VMEM((HI, 8, 2 * W), F32),
            pltpu.VMEM((S * C, W), F32),
            pltpu.VMEM((S * C, W), F32),
            pltpu.VMEM((S * C, W), F32),
            pltpu.VMEM((TAPS, S * C, W), F32),
            pltpu.VMEM((S * C, 2 * W), F32),
            pltpu.VMEM((S * C, 2 * W), F32),
            pltpu.VMEM((S * C, 2 * W), F32),
        ]
        + [pltpu.VMEM(x.shape, x.dtype) for x in operands]
        + [pltpu.VMEM((2, S, W), F32)]
        + [
            pltpu.SemaphoreType.DMA((SEMAPHORES,)),
            pltpu.SemaphoreType.DMA((SEMAPHORES,)),
            pltpu.SemaphoreType.DMA((len(operands),)),
        ],
        compiler_params=pltpu.CompilerParams(
            collective_id=0, has_side_effects=True, vmem_limit_bytes=VMEM_BYTES
        ),
        name="exchange",
    )(*operands)
    *streams, tap_sums = pl.pallas_call(
        write_kernel,
        out_shape=(stream, stream, stream, filt, tap_rows),
        in_specs=[vmem] * 6,
        out_specs=(hbm,) * 5,
        scratch_shapes=[pltpu.SemaphoreType.DMA((6,))],
        compiler_params=pltpu.CompilerParams(vmem_limit_bytes=WRITE_BYTES),
        name="write",
    )(*outs)
    return (*streams, tap_sums.T)


def solution(mesh):
    spec = P("chan", "seq")
    owned = P(("chan", "seq"), None)
    taps = P("chan", None)
    return jax.shard_map(
        on_device,
        mesh=mesh,
        in_specs=(spec, spec, spec, spec, owned, taps),
        out_specs=(spec, spec, spec, owned, taps),
        check_vma=False,
    )
```

```python
import math

import jax
import jax.numpy as jnp
import ml_dtypes
import numpy as np
from jax import lax
from jax.experimental import pallas as pl
from jax.experimental.pallas import tpu as pltpu
from jax.sharding import PartitionSpec as P

TAPS = 3
MESH = pl.DeviceIdType.MESH
BF = jnp.bfloat16
F32 = jnp.float32

S = 64
W = 128
C = 8
N = S * W
PLANE = 16
HI = 4
PARTS = (range(0, 4), range(4, 6), range(6, 8))
WHOLE = range(C)
PLANE_SUM, HEIGHT_SUM, VALUE_HALO, GRAD_HALO, MIXED, CONV, GRAD = range(7)
BACK = GRAD + len(PARTS)
SEMAPHORES = BACK + len(PARTS)
VMEM_BYTES = 55_820_000
WRITE_BYTES = 4_000_000


def halves(table):
    hi = table.astype(ml_dtypes.bfloat16)
    lo = (table - hi.astype(np.float64)).astype(ml_dtypes.bfloat16)
    return hi, lo


def tables():
    quarter = np.arange(S) + 0.25
    rows = 2.0 * np.pi * np.outer(quarter, np.arange(S)) / S
    twist = 2.0 * np.pi * np.outer(quarter, np.arange(W)) / N
    cols = 2.0 * np.pi * np.outer(np.arange(W), np.arange(W)) / W
    a_hi, a_lo = halves(np.concatenate([np.cos(rows), -np.sin(rows)], axis=0))
    b_hi, b_lo = halves(np.concatenate([np.cos(rows).T, -np.sin(rows).T], axis=1) / N)
    fr, fi = np.cos(cols), -np.sin(cols)
    f_hi, f_lo = halves(np.block([[fr, fi], [-fi, fr]]))
    g_hi, g_lo = halves(np.block([[fr, -fi], [fi, fr]]))
    turn = np.concatenate([np.cos(twist), -np.sin(twist)], axis=1)
    turn_hi, turn_lo = halves(turn)
    turn_rest = (turn - turn_hi.astype(np.float64) - turn_lo.astype(np.float64)).astype(ml_dtypes.bfloat16)
    return np.concatenate(
        [
            f_hi, f_lo, g_hi, g_lo,
            np.concatenate([a_hi, a_lo, a_hi, a_lo], axis=1),
            np.concatenate([b_hi, b_lo], axis=1), turn_hi, turn_lo, turn_rest,
        ],
        axis=0,
    )


def split(x):
    hi = x.astype(BF)
    return hi, (x - hi.astype(F32)).astype(BF)


def dot(a, b):
    return jnp.dot(a, b, preferred_element_type=F32)


def to_rows(x):
    return jnp.concatenate([x[:, i : i + W] for i in range(0, x.shape[1], W)], axis=0)


def to_cols(x):
    return jnp.concatenate([x[i : i + S] for i in range(0, x.shape[0], S)], axis=1)


def wide(table, like):
    return jnp.concatenate([table] * (like.shape[1] // W), axis=1)


def forward(stacked, first, middle, turn):
    y = dot(first, stacked)
    yr, yi = y[:S], y[S:]
    tc, ts = wide(turn[0], yr), wide(turn[1], yr)
    turned = jnp.concatenate([to_rows(yr * tc - yi * ts), to_rows(yr * ts + yi * tc)], axis=1)
    hi, lo = split(turned)
    return dot(hi, middle(0)) + dot(lo, middle(0)) + dot(hi, middle(1))


def inverse(spec_re, spec_im, middle, last, turn):
    hi, lo = split(jnp.concatenate([spec_re, spec_im], axis=1))
    v = dot(hi, middle(2)) + dot(lo, middle(2)) + dot(hi, middle(3))
    vr, vi = to_cols(v[:, :W]), to_cols(v[:, W:])
    tc, ts = wide(turn[0], vr), wide(turn[1], vr)
    hi, lo = split(jnp.concatenate([vr * tc + vi * ts, vi * tc - vr * ts], axis=0))
    return dot(last(), jnp.concatenate([hi, hi, lo], axis=0))


def load_signal(ref, channels):
    return jnp.concatenate([ref[pl.ds(c, S, stride=C), :] for c in channels], axis=1)


def store_signal(ref, x, channels):
    for i, c in enumerate(channels):
        ref[pl.ds(c, S, stride=C), :] = x[:, i * W : (i + 1) * W]


def row_pick(rows, lanes):
    r = lax.broadcasted_iota(jnp.int32, (8, W), 0)
    l = lax.broadcasted_iota(jnp.int32, (8, W), 1)
    hit = None
    for row, lane in zip(rows, lanes):
        one = (r == row) & (l == lane)
        hit = one if hit is None else hit | one
    return hit.astype(F32)


def pack_pair(x, lanes):
    total = None
    for b in range(4):
        part = lax.dot_general(
            row_pick((2 * b, 2 * b + 1), lanes).astype(BF),
            x[b * W : (b + 1) * W],
            (((1,), (1,)), ((), ())),
            preferred_element_type=F32,
        )
        total = part if total is None else total + part
    return total


def unpack_pair(packed, lanes):
    turned = packed.T.astype(BF)
    return jnp.concatenate(
        [dot(turned, row_pick((2 * b, 2 * b + 1), lanes).astype(BF)) for b in range(4)], axis=0
    )


def main_kernel(
    q_hbm, k_hbm, v_hbm, cot_hbm, h_hbm, a_hbm, table_hbm,
    qg_ref, kg_ref, vg_ref, fg_ref, fg_more, tg_ref,
    g_out, g_in, m_out, m_in, b_out, b_in, c_out, c_in,
    vh_out, vh_in, fh_out, fh_in, tp_out, tp_in, tz_out, tz_in,
    rows_ref, filt_ref, low_ref, lag_ref, hs_ref, gs_ref, ms_ref,
    q_ref, k_ref, v_ref, cot_ref, h_ref, a_ref, table_ref, turn_ref,
    send_sems, recv_sems, load_sems,
):
    loads = [
        pltpu.make_async_copy(src, dst, load_sems.at[i])
        for i, (src, dst) in enumerate((
            (h_hbm, h_ref), (table_hbm, table_ref), (cot_hbm, cot_ref), (q_hbm, q_ref),
            (v_hbm, v_ref), (a_hbm, a_ref), (k_hbm, k_ref),
        ))
    ]
    me = lax.axis_index("seq")
    after, before = lax.rem(me + 1, S), lax.rem(me + S - 1, S)
    barrier = pltpu.get_barrier_semaphore()

    place, height = lax.rem(me, PLANE), me // PLANE

    def to_all(act):
        heights = [lax.rem(height + h, HI) * PLANE for h in (2, 1, 3, 0)]
        for base in heights[:3]:
            act(base + place)

        def one(i, carry):
            at = lax.rem(place + i, PLANE)
            for base in heights:
                act(base + at)
            return carry

        lax.fori_loop(1, PLANE, one, 0)

    to_all(
        lambda to: pl.semaphore_signal(barrier, inc=1, device_id={"seq": to}, device_id_type=MESH)
    )
    for load in loads:
        load.start()

    def remote(src, dst, index, to):
        return pltpu.make_async_remote_copy(
            src_ref=src, dst_ref=dst, send_sem=send_sems.at[index], recv_sem=recv_sems.at[index],
            device_id={"seq": to}, device_id_type=MESH,
        )

    def exchange(out, into, index, channels):
        part = pl.ds(channels[0], len(channels))
        to_all(lambda to: remote(out.at[to, part], into.at[me, part], index, to).start())
        into[me, part] = out[me, part]

    def arrived(buffer, sem, count):
        part = buffer.at[pl.ds(0, count)]
        pltpu.make_async_copy(part, part, sem).wait()

    def exchanged(buffer, sem, channels):
        part = buffer.at[pl.ds(0, S - 1), pl.ds(channels[0], len(channels))]
        pltpu.make_async_copy(part, part, sem).wait()

    first = table_ref.at[pl.ds(1024, 2 * S)]
    turn = turn_ref

    def mid_ref(i):
        return table_ref[256 * i : 256 * (i + 1), :]

    def last_ref():
        back = table_ref[1152 : 1152 + S, :]
        return jnp.concatenate([back, back[:, : 2 * S]], axis=1)

    tiles_ref = rows_ref.reshape(S, C, W)

    with jax.named_scope("local"):
        for load in loads:
            load.wait()
        pieces = [table_ref[1216 + i * S : 1216 + (i + 1) * S, :].astype(F32) for i in range(3)]
        turned = pieces[0] + pieces[1] + pieces[2]
        turn_ref[0] = turned[:, :W]
        turn_ref[1] = turned[:, W:]
        cot = cot_ref[...].astype(F32)
        g_out[...] = (cot * q_ref[...].astype(F32)).astype(BF).reshape(S, C, W)
        vh_out[...] = pack_pair(v_ref[...], (W - 2, W - 1))
        for n in range(S):
            rows_ref[n * C : (n + 1) * C, :] = h_ref[:, n * W : (n + 1) * W]
        hi, lo = split(load_signal(rows_ref, range(C)))
        hs_ref[...] = forward(jnp.concatenate([hi, hi, lo, lo], axis=0), first[...], mid_ref, turn)

    with jax.named_scope("wait_barrier"):
        pl.semaphore_wait(barrier, S - 1)

    halo_v = remote(vh_out, vh_in, VALUE_HALO, after)
    halo_v.start()
    with jax.named_scope("send_g"):
        for i, channels in enumerate(PARTS):
            exchange(g_out, g_in, GRAD + i, channels)

    value = v_ref[...].astype(F32)
    a_all = a_ref[...]
    taps = jnp.concatenate(
        [
            jnp.concatenate([a_all[:, b * W : (b + 1) * W], jnp.zeros((8 - TAPS, W), F32)], axis=0).T
            for b in range(4)
        ],
        axis=0,
    )
    with jax.named_scope("wait_halo_v"):
        halo_v.wait()
    held = jnp.where(me > 0, vh_in[...], 0.0)
    value_prev = unpack_pair(held, (W - 2, W - 1))
    lane = lax.broadcasted_iota(jnp.int32, (C * S, W), 1)

    def lagged(j):
        return jnp.where(lane < j, pltpu.roll(value_prev, j, 1), pltpu.roll(value, j, 1))

    filtered = taps[:, 0:1] * value
    lag_ref[0] = value
    for j in range(1, TAPS):
        lag_ref[j] = lagged(j)
        filtered = filtered + taps[:, j : j + 1] * lag_ref[j]
    filt_ref[...] = filtered
    m_out[...] = (k_ref[...].astype(F32) * filtered).astype(BF).reshape(S, C, W)
    with jax.named_scope("send_m"):
        exchange(m_out, m_in, MIXED, WHOLE)

    def take(buffer, channels):
        part = pl.ds(channels[0], len(channels))
        tiles_ref[:, part, :] = buffer[:, part, :].astype(F32)
        x = load_signal(rows_ref, channels).astype(BF)
        return forward(jnp.concatenate([x, x], axis=0), first[:, : 2 * S], mid_ref, turn)

    def give(buffer, x, channels):
        part = pl.ds(channels[0], len(channels))
        store_signal(rows_ref, x, channels)
        buffer[:, part, :] = tiles_ref[:, part, :].astype(BF)

    for i, channels in enumerate(PARTS):
        with jax.named_scope("wait_g"):
            exchanged(g_in, recv_sems.at[GRAD + i], channels)
        grad = take(g_in, channels)
        mine = pl.ds(channels[0] * S, len(channels) * S)
        gs_ref[mine, :] = grad
        hs = hs_ref[mine, :]
        hr, hi_ = hs[:, :W], hs[:, W:]
        gr, gi = grad[:, :W], grad[:, W:]
        back = inverse(hr * gr + hi_ * gi, hr * gi - hi_ * gr, mid_ref, last_ref, turn)
        give(b_out, back, channels)
        with jax.named_scope("send_b"):
            exchange(b_out, b_in, BACK + i, channels)

    with jax.named_scope("wait_m"):
        exchanged(m_in, recv_sems.at[MIXED], WHOLE)
    mixed = take(m_in, WHOLE)
    ms_ref[...] = mixed
    hs = hs_ref[...]
    hr, hi_ = hs[:, :W], hs[:, W:]
    mr, mi = mixed[:, :W], mixed[:, W:]
    conv = inverse(mr * hr - mi * hi_, mr * hi_ + mi * hr, mid_ref, last_ref, turn)
    give(c_out, conv, WHOLE)
    with jax.named_scope("send_c"):
        exchange(c_out, c_in, CONV, WHOLE)

    with jax.named_scope("wait_b"):
        for i, channels in enumerate(PARTS):
            exchanged(b_in, recv_sems.at[BACK + i], channels)
    back = b_in[...].astype(F32).reshape(S * C, W)
    low_bf = (back * k_ref[...].astype(F32)).astype(BF)
    low_ref[...] = low_bf.astype(F32)
    low = low_ref[...]
    row8 = lax.broadcasted_iota(jnp.int32, (8, W), 0)
    partial = jnp.zeros((8, 2 * W), F32)
    for j in range(TAPS):
        pieces = split(low * lag_ref[j])
        for half in range(2):
            mark = (row8 == 4 * half + j).astype(BF)
            for piece in pieces:
                partial = partial + lax.dot_general(
                    mark, piece[half * 2 * W : (half + 1) * 2 * W], (((1,), (1,)), ((), ())),
                    preferred_element_type=F32,
                )
    tp_out[...] = partial
    def to_plane(i, carry):
        to = height * PLANE + lax.rem(place + i, PLANE)
        remote(tp_out, tp_in.at[place], PLANE_SUM, to).start()
        return carry

    with jax.named_scope("send_tp"):
        lax.fori_loop(1, PLANE, to_plane, 0)
    tp_in[place] = tp_out[...]

    fh_out[...] = pack_pair(low_bf, (0, 1))
    halo_f = remote(fh_out, fh_in, GRAD_HALO, before)
    halo_f.start()
    kg_ref[...] = (b_in[...].astype(F32).reshape(S * C, W) * filt_ref[...]).astype(BF)

    mixed, grad = ms_ref[...], gs_ref[...]
    mr, mi = mixed[:, :W], mixed[:, W:]
    gr, gi = grad[:, :W], grad[:, W:]
    fg = inverse(mr * gr + mi * gi, mr * gi - mi * gr, mid_ref, last_ref, turn)
    store_signal(rows_ref, fg * (1.0 / math.sqrt(N)), range(C))
    for n in range(S):
        part, at = (fg_ref, n * W) if n < S // 2 else (fg_more, (n - S // 2) * W)
        part[:, at : at + W] = rows_ref[n * C : (n + 1) * C, :]

    with jax.named_scope("wait_tp"):
        arrived(tp_in, recv_sems.at[PLANE_SUM], PLANE - 1)
    tz_out[...] = jnp.sum(tp_in[...], axis=0)

    def to_heights(i, carry):
        to = lax.rem(height + i, HI) * PLANE + place
        remote(tz_out, tz_in.at[height], HEIGHT_SUM, to).start()
        return carry

    lax.fori_loop(1, HI, to_heights, 0)
    tz_in[height] = tz_out[...]

    with jax.named_scope("wait_halo_f"):
        halo_f.wait()
    held = jnp.where(me < S - 1, fh_in[...], 0.0)
    low_next = unpack_pair(held, (0, 1))
    value_grad = taps[:, 0:1] * low
    for j in range(1, TAPS):
        ahead = jnp.where(lane >= W - j, pltpu.roll(low_next, W - j, 1), pltpu.roll(low, W - j, 1))
        value_grad = value_grad + taps[:, j : j + 1] * ahead
    vg_ref[...] = value_grad.astype(BF)

    with jax.named_scope("wait_c"):
        exchanged(c_in, recv_sems.at[CONV], WHOLE)
    conv = c_in[...].astype(F32).reshape(S * C, W)
    qg_ref[...] = (cot_ref[...].astype(F32) * conv).astype(BF)

    with jax.named_scope("wait_tz"):
        arrived(tz_in, recv_sems.at[HEIGHT_SUM], HI - 1)
    sums = jnp.sum(tz_in[...], axis=0) * (1.0 / math.sqrt(N))
    tg_ref[:, : 2 * W] = sums[:TAPS]
    tg_ref[:, 2 * W :] = sums[4 : 4 + TAPS]

    for i, channels in enumerate(PARTS):
        exchanged(g_out, send_sems.at[GRAD + i], channels)
        exchanged(b_out, send_sems.at[BACK + i], channels)
    exchanged(m_out, send_sems.at[MIXED], WHOLE)
    exchanged(c_out, send_sems.at[CONV], WHOLE)
    arrived(tp_in, send_sems.at[PLANE_SUM], PLANE - 1)
    arrived(tz_in, send_sems.at[HEIGHT_SUM], HI - 1)


def write_kernel(qg, kg, vg, fg, fg_more, tg, qg_out, kg_out, vg_out, fg_out, tg_out, sems):
    pairs = (
        (qg, qg_out), (kg, kg_out), (vg, vg_out), (tg, tg_out),
        (fg, fg_out.at[:, pl.ds(0, N // 2)]), (fg_more, fg_out.at[:, pl.ds(N // 2, N // 2)]),
    )
    copies = [pltpu.make_async_copy(src, dst, sems.at[i]) for i, (src, dst) in enumerate(pairs)]
    for copy in copies:
        copy.start()
    for copy in copies:
        copy.wait()


def on_device(query_gate, key_gate, value_in, cotangent, long_filter, short_taps):
    rows, width = key_gate.shape
    table = jnp.asarray(tables())
    hbm = pl.BlockSpec(memory_space=pltpu.HBM)
    vmem = pl.BlockSpec(memory_space=pltpu.VMEM)
    stream = jax.ShapeDtypeStruct((rows, width), BF)
    filt = jax.ShapeDtypeStruct((C, N), F32)
    half = jax.ShapeDtypeStruct((C, N // 2), F32)
    tap_rows = jax.ShapeDtypeStruct((TAPS, rows), F32)
    operands = (query_gate, key_gate, value_in, cotangent, long_filter, short_taps.T, table)
    outs = pl.pallas_call(
        main_kernel,
        out_shape=(stream, stream, stream, half, half, tap_rows),
        in_specs=[hbm] * len(operands),
        out_specs=(vmem,) * 6,
        scratch_shapes=[pltpu.VMEM((S, C, W), BF)] * 8
        + [pltpu.VMEM((8, W), F32)] * 4
        + [
            pltpu.VMEM((8, 2 * W), F32),
            pltpu.VMEM((PLANE, 8, 2 * W), F32),
            pltpu.VMEM((8, 2 * W), F32),
            pltpu.VMEM((HI, 8, 2 * W), F32),
            pltpu.VMEM((S * C, W), F32),
            pltpu.VMEM((S * C, W), F32),
            pltpu.VMEM((S * C, W), F32),
            pltpu.VMEM((TAPS, S * C, W), F32),
            pltpu.VMEM((S * C, 2 * W), F32),
            pltpu.VMEM((S * C, 2 * W), F32),
            pltpu.VMEM((S * C, 2 * W), F32),
        ]
        + [pltpu.VMEM(x.shape, x.dtype) for x in operands]
        + [pltpu.VMEM((2, S, W), F32)]
        + [
            pltpu.SemaphoreType.DMA((SEMAPHORES,)),
            pltpu.SemaphoreType.DMA((SEMAPHORES,)),
            pltpu.SemaphoreType.DMA((len(operands),)),
        ],
        compiler_params=pltpu.CompilerParams(
            collective_id=0, has_side_effects=True, vmem_limit_bytes=VMEM_BYTES
        ),
        name="exchange",
    )(*operands)
    *streams, tap_sums = pl.pallas_call(
        write_kernel,
        out_shape=(stream, stream, stream, filt, tap_rows),
        in_specs=[vmem] * 6,
        out_specs=(hbm,) * 5,
        scratch_shapes=[pltpu.SemaphoreType.DMA((6,))],
        compiler_params=pltpu.CompilerParams(vmem_limit_bytes=WRITE_BYTES),
        name="write",
    )(*outs)
    return (*streams, tap_sums.T)


def solution(mesh):
    spec = P("chan", "seq")
    owned = P(("chan", "seq"), None)
    taps = P("chan", None)
    return jax.shard_map(
        on_device,
        mesh=mesh,
        in_specs=(spec, spec, spec, spec, owned, taps),
        out_specs=(spec, spec, spec, owned, taps),
        check_vma=False,
    )
```

```python
import math

import jax
import jax.numpy as jnp
import ml_dtypes
import numpy as np
from jax import lax
from jax.experimental import pallas as pl
from jax.experimental.pallas import tpu as pltpu
from jax.sharding import PartitionSpec as P

TAPS = 3
MESH = pl.DeviceIdType.MESH
BF = jnp.bfloat16
F32 = jnp.float32

S = 64
W = 128
C = 8
N = S * W
PLANE = 16
HI = 4
PARTS = (range(0, 4), range(4, 6), range(6, 8))
WHOLE = range(C)
PLANE_SUM, HEIGHT_SUM, VALUE_HALO, GRAD_HALO, MIXED, CONV, GRAD = range(7)
BACK = GRAD + len(PARTS)
SEMAPHORES = BACK + len(PARTS)
VMEM_BYTES = 55_820_000
WRITE_BYTES = 4_000_000


def halves(table):
    hi = table.astype(ml_dtypes.bfloat16)
    lo = (table - hi.astype(np.float64)).astype(ml_dtypes.bfloat16)
    return hi, lo


def tables():
    quarter = np.arange(S) + 0.25
    rows = 2.0 * np.pi * np.outer(quarter, np.arange(S)) / S
    twist = 2.0 * np.pi * np.outer(quarter, np.arange(W)) / N
    cols = 2.0 * np.pi * np.outer(np.arange(W), np.arange(W)) / W
    a_hi, a_lo = halves(np.concatenate([np.cos(rows), -np.sin(rows)], axis=0))
    b_hi, b_lo = halves(np.concatenate([np.cos(rows).T, -np.sin(rows).T], axis=1) / N)
    fr, fi = np.cos(cols), -np.sin(cols)
    f_hi, f_lo = halves(np.block([[fr, fi], [-fi, fr]]))
    g_hi, g_lo = halves(np.block([[fr, -fi], [fi, fr]]))
    turn = np.concatenate([np.cos(twist), -np.sin(twist)], axis=1)
    turn_hi, turn_lo = halves(turn)
    turn_rest = (turn - turn_hi.astype(np.float64) - turn_lo.astype(np.float64)).astype(ml_dtypes.bfloat16)
    return np.concatenate(
        [
            f_hi, f_lo, g_hi, g_lo,
            np.concatenate([a_hi, a_lo, a_hi, a_lo], axis=1),
            np.concatenate([b_hi, b_lo], axis=1), turn_hi, turn_lo, turn_rest,
        ],
        axis=0,
    )


def split(x):
    hi = x.astype(BF)
    return hi, (x - hi.astype(F32)).astype(BF)


def dot(a, b):
    return jnp.dot(a, b, preferred_element_type=F32)


def to_rows(x):
    return jnp.concatenate([x[:, i : i + W] for i in range(0, x.shape[1], W)], axis=0)


def to_cols(x):
    return jnp.concatenate([x[i : i + S] for i in range(0, x.shape[0], S)], axis=1)


def wide(table, like):
    return jnp.concatenate([table] * (like.shape[1] // W), axis=1)


def forward(stacked, first, middle, turn):
    y = dot(first, stacked)
    yr, yi = y[:S], y[S:]
    tc, ts = wide(turn[0], yr), wide(turn[1], yr)
    turned = jnp.concatenate([to_rows(yr * tc - yi * ts), to_rows(yr * ts + yi * tc)], axis=1)
    hi, lo = split(turned)
    return dot(hi, middle(0)) + dot(lo, middle(0)) + dot(hi, middle(1))


def inverse(spec_re, spec_im, middle, last, turn):
    hi, lo = split(jnp.concatenate([spec_re, spec_im], axis=1))
    v = dot(hi, middle(2)) + dot(lo, middle(2)) + dot(hi, middle(3))
    vr, vi = to_cols(v[:, :W]), to_cols(v[:, W:])
    tc, ts = wide(turn[0], vr), wide(turn[1], vr)
    hi, lo = split(jnp.concatenate([vr * tc + vi * ts, vi * tc - vr * ts], axis=0))
    return dot(last(), jnp.concatenate([hi, hi, lo], axis=0))


def load_signal(ref, channels):
    return jnp.concatenate([ref[pl.ds(c, S, stride=C), :] for c in channels], axis=1)


def store_signal(ref, x, channels):
    for i, c in enumerate(channels):
        ref[pl.ds(c, S, stride=C), :] = x[:, i * W : (i + 1) * W]


def row_pick(rows, lanes):
    r = lax.broadcasted_iota(jnp.int32, (8, W), 0)
    l = lax.broadcasted_iota(jnp.int32, (8, W), 1)
    hit = None
    for row, lane in zip(rows, lanes):
        one = (r == row) & (l == lane)
        hit = one if hit is None else hit | one
    return hit.astype(F32)


def pack_pair(x, lanes):
    total = None
    for b in range(4):
        part = lax.dot_general(
            row_pick((2 * b, 2 * b + 1), lanes).astype(BF),
            x[b * W : (b + 1) * W],
            (((1,), (1,)), ((), ())),
            preferred_element_type=F32,
        )
        total = part if total is None else total + part
    return total


def unpack_pair(packed, lanes):
    turned = packed.T.astype(BF)
    return jnp.concatenate(
        [dot(turned, row_pick((2 * b, 2 * b + 1), lanes).astype(BF)) for b in range(4)], axis=0
    )


def main_kernel(
    q_hbm, k_hbm, v_hbm, cot_hbm, h_hbm, a_hbm, table_hbm,
    qg_ref, kg_ref, vg_ref, fg_ref, fg_more, tg_ref,
    g_out, g_in, m_out, m_in, b_out, b_in, c_out, c_in,
    vh_out, vh_in, fh_out, fh_in, tp_out, tp_in, tz_out, tz_in,
    rows_ref, filt_ref, low_ref, lag_ref, hs_ref, gs_ref, ms_ref,
    q_ref, k_ref, v_ref, cot_ref, h_ref, a_ref, table_ref, turn_ref,
    send_sems, recv_sems, load_sems,
):
    loads = [
        pltpu.make_async_copy(src, dst, load_sems.at[i])
        for i, (src, dst) in enumerate((
            (h_hbm, h_ref), (table_hbm, table_ref), (cot_hbm, cot_ref), (q_hbm, q_ref),
            (v_hbm, v_ref), (a_hbm, a_ref), (k_hbm, k_ref),
        ))
    ]
    me = lax.axis_index("seq")
    after, before = lax.rem(me + 1, S), lax.rem(me + S - 1, S)
    barrier = pltpu.get_barrier_semaphore()

    place, height = lax.rem(me, PLANE), me // PLANE

    def to_all(act):
        heights = [lax.rem(height + h, HI) * PLANE for h in (2, 1, 3, 0)]
        for base in heights[:3]:
            act(base + place)

        def one(i, carry):
            at = lax.rem(place + i, PLANE)
            for base in heights:
                act(base + at)
            return carry

        lax.fori_loop(1, PLANE, one, 0)

    to_all(
        lambda to: pl.semaphore_signal(barrier, inc=1, device_id={"seq": to}, device_id_type=MESH)
    )
    for load in loads:
        load.start()

    def remote(src, dst, index, to):
        return pltpu.make_async_remote_copy(
            src_ref=src, dst_ref=dst, send_sem=send_sems.at[index], recv_sem=recv_sems.at[index],
            device_id={"seq": to}, device_id_type=MESH,
        )

    def exchange(out, into, index, channels):
        part = pl.ds(channels[0], len(channels))
        to_all(lambda to: remote(out.at[to, part], into.at[me, part], index, to).start())
        into[me, part] = out[me, part]

    def arrived(buffer, sem, count):
        part = buffer.at[pl.ds(0, count)]
        pltpu.make_async_copy(part, part, sem).wait()

    def exchanged(buffer, sem, channels):
        part = buffer.at[pl.ds(0, S - 1), pl.ds(channels[0], len(channels))]
        pltpu.make_async_copy(part, part, sem).wait()

    first = table_ref.at[pl.ds(1024, 2 * S)]
    turn = turn_ref

    def mid_ref(i):
        return table_ref[256 * i : 256 * (i + 1), :]

    def last_ref():
        back = table_ref[1152 : 1152 + S, :]
        return jnp.concatenate([back, back[:, : 2 * S]], axis=1)

    tiles_ref = rows_ref.reshape(S, C, W)

    with jax.named_scope("local"):
        for load in loads:
            load.wait()
        pieces = [table_ref[1216 + i * S : 1216 + (i + 1) * S, :].astype(F32) for i in range(3)]
        turned = pieces[0] + pieces[1] + pieces[2]
        turn_ref[0] = turned[:, :W]
        turn_ref[1] = turned[:, W:]
        cot = cot_ref[...].astype(F32)
        g_out[...] = (cot * q_ref[...].astype(F32)).astype(BF).reshape(S, C, W)
        vh_out[...] = pack_pair(v_ref[...], (W - 2, W - 1))
        for n in range(S):
            rows_ref[n * C : (n + 1) * C, :] = h_ref[:, n * W : (n + 1) * W]
        hi, lo = split(load_signal(rows_ref, range(C)))
        hs_ref[...] = forward(jnp.concatenate([hi, hi, lo, lo], axis=0), first[...], mid_ref, turn)

    with jax.named_scope("wait_barrier"):
        pl.semaphore_wait(barrier, S - 1)

    halo_v = remote(vh_out, vh_in, VALUE_HALO, after)
    halo_v.start()
    with jax.named_scope("send_g"):
        for i, channels in enumerate(PARTS):
            exchange(g_out, g_in, GRAD + i, channels)

    value = v_ref[...].astype(F32)
    a_all = a_ref[...]
    taps = jnp.concatenate(
        [
            jnp.concatenate([a_all[:, b * W : (b + 1) * W], jnp.zeros((8 - TAPS, W), F32)], axis=0).T
            for b in range(4)
        ],
        axis=0,
    )
    with jax.named_scope("wait_halo_v"):
        halo_v.wait()
    held = jnp.where(me > 0, vh_in[...], 0.0)
    value_prev = unpack_pair(held, (W - 2, W - 1))
    lane = lax.broadcasted_iota(jnp.int32, (C * S, W), 1)

    def lagged(j):
        return jnp.where(lane < j, pltpu.roll(value_prev, j, 1), pltpu.roll(value, j, 1))

    filtered = taps[:, 0:1] * value
    lag_ref[0] = value
    for j in range(1, TAPS):
        lag_ref[j] = lagged(j)
        filtered = filtered + taps[:, j : j + 1] * lag_ref[j]
    filt_ref[...] = filtered
    m_out[...] = (k_ref[...].astype(F32) * filtered).astype(BF).reshape(S, C, W)
    with jax.named_scope("send_m"):
        exchange(m_out, m_in, MIXED, WHOLE)

    def take(buffer, channels):
        part = pl.ds(channels[0], len(channels))
        tiles_ref[:, part, :] = buffer[:, part, :].astype(F32)
        x = load_signal(rows_ref, channels).astype(BF)
        return forward(jnp.concatenate([x, x], axis=0), first[:, : 2 * S], mid_ref, turn)

    def give(buffer, x, channels):
        part = pl.ds(channels[0], len(channels))
        store_signal(rows_ref, x, channels)
        buffer[:, part, :] = tiles_ref[:, part, :].astype(BF)

    for i, channels in enumerate(PARTS):
        with jax.named_scope("wait_g"):
            exchanged(g_in, recv_sems.at[GRAD + i], channels)
        grad = take(g_in, channels)
        mine = pl.ds(channels[0] * S, len(channels) * S)
        gs_ref[mine, :] = grad
        hs = hs_ref[mine, :]
        hr, hi_ = hs[:, :W], hs[:, W:]
        gr, gi = grad[:, :W], grad[:, W:]
        back = inverse(hr * gr + hi_ * gi, hr * gi - hi_ * gr, mid_ref, last_ref, turn)
        give(b_out, back, channels)
        with jax.named_scope("send_b"):
            exchange(b_out, b_in, BACK + i, channels)

    with jax.named_scope("wait_m"):
        exchanged(m_in, recv_sems.at[MIXED], WHOLE)
    mixed = take(m_in, WHOLE)
    ms_ref[...] = mixed
    hs = hs_ref[...]
    hr, hi_ = hs[:, :W], hs[:, W:]
    mr, mi = mixed[:, :W], mixed[:, W:]
    conv = inverse(mr * hr - mi * hi_, mr * hi_ + mi * hr, mid_ref, last_ref, turn)
    give(c_out, conv, WHOLE)
    with jax.named_scope("send_c"):
        exchange(c_out, c_in, CONV, WHOLE)

    mixed, grad = ms_ref[...], gs_ref[...]
    mr, mi = mixed[:, :W], mixed[:, W:]
    gr, gi = grad[:, :W], grad[:, W:]
    fg = inverse(mr * gr + mi * gi, mr * gi - mi * gr, mid_ref, last_ref, turn)
    store_signal(rows_ref, fg * (1.0 / math.sqrt(N)), range(C))
    for n in range(S):
        part, at = (fg_ref, n * W) if n < S // 2 else (fg_more, (n - S // 2) * W)
        part[:, at : at + W] = rows_ref[n * C : (n + 1) * C, :]

    with jax.named_scope("wait_b"):
        for i, channels in enumerate(PARTS):
            exchanged(b_in, recv_sems.at[BACK + i], channels)
    back = b_in[...].astype(F32).reshape(S * C, W)
    low_bf = (back * k_ref[...].astype(F32)).astype(BF)
    low_ref[...] = low_bf.astype(F32)
    low = low_ref[...]
    row8 = lax.broadcasted_iota(jnp.int32, (8, W), 0)
    partial = jnp.zeros((8, 2 * W), F32)
    for j in range(TAPS):
        pieces = split(low * lag_ref[j])
        for half in range(2):
            mark = (row8 == 4 * half + j).astype(BF)
            for piece in pieces:
                partial = partial + lax.dot_general(
                    mark, piece[half * 2 * W : (half + 1) * 2 * W], (((1,), (1,)), ((), ())),
                    preferred_element_type=F32,
                )
    tp_out[...] = partial
    with jax.named_scope("send_tp"):
        steps = [(dx, dy) for dx in range(4) for dy in range(4) if dx or dy]
        for dx, dy in sorted(steps, key=lambda d: -sum(min(n, 4 - n) for n in d)):
            at = lax.rem(place // 4 + dx, 4) * 4 + lax.rem(place + dy, 4)
            remote(tp_out, tp_in.at[place], PLANE_SUM, height * PLANE + at).start()
    tp_in[place] = tp_out[...]

    fh_out[...] = pack_pair(low_bf, (0, 1))
    halo_f = remote(fh_out, fh_in, GRAD_HALO, before)
    halo_f.start()
    kg_ref[...] = (b_in[...].astype(F32).reshape(S * C, W) * filt_ref[...]).astype(BF)

    with jax.named_scope("wait_tp"):
        arrived(tp_in, recv_sems.at[PLANE_SUM], PLANE - 1)
    tz_out[...] = jnp.sum(tp_in[...], axis=0)

    for h in (2, 1, 3):
        to = lax.rem(height + h, HI) * PLANE + place
        remote(tz_out, tz_in.at[height], HEIGHT_SUM, to).start()
    tz_in[height] = tz_out[...]

    with jax.named_scope("wait_halo_f"):
        halo_f.wait()
    held = jnp.where(me < S - 1, fh_in[...], 0.0)
    low_next = unpack_pair(held, (0, 1))
    value_grad = taps[:, 0:1] * low
    for j in range(1, TAPS):
        ahead = jnp.where(lane >= W - j, pltpu.roll(low_next, W - j, 1), pltpu.roll(low, W - j, 1))
        value_grad = value_grad + taps[:, j : j + 1] * ahead
    vg_ref[...] = value_grad.astype(BF)

    with jax.named_scope("wait_c"):
        exchanged(c_in, recv_sems.at[CONV], WHOLE)
    conv = c_in[...].astype(F32).reshape(S * C, W)
    qg_ref[...] = (cot_ref[...].astype(F32) * conv).astype(BF)

    with jax.named_scope("wait_tz"):
        arrived(tz_in, recv_sems.at[HEIGHT_SUM], HI - 1)
    sums = jnp.sum(tz_in[...], axis=0) * (1.0 / math.sqrt(N))
    tg_ref[:, : 2 * W] = sums[:TAPS]
    tg_ref[:, 2 * W :] = sums[4 : 4 + TAPS]

    for i, channels in enumerate(PARTS):
        exchanged(g_out, send_sems.at[GRAD + i], channels)
        exchanged(b_out, send_sems.at[BACK + i], channels)
    exchanged(m_out, send_sems.at[MIXED], WHOLE)
    exchanged(c_out, send_sems.at[CONV], WHOLE)
    arrived(tp_in, send_sems.at[PLANE_SUM], PLANE - 1)
    arrived(tz_in, send_sems.at[HEIGHT_SUM], HI - 1)


def write_kernel(qg, kg, vg, fg, fg_more, tg, qg_out, kg_out, vg_out, fg_out, tg_out, sems):
    pairs = (
        (qg, qg_out), (kg, kg_out), (vg, vg_out), (tg, tg_out),
        (fg, fg_out.at[:, pl.ds(0, N // 2)]), (fg_more, fg_out.at[:, pl.ds(N // 2, N // 2)]),
    )
    copies = [pltpu.make_async_copy(src, dst, sems.at[i]) for i, (src, dst) in enumerate(pairs)]
    for copy in copies:
        copy.start()
    for copy in copies:
        copy.wait()


def on_device(query_gate, key_gate, value_in, cotangent, long_filter, short_taps):
    rows, width = key_gate.shape
    table = jnp.asarray(tables())
    hbm = pl.BlockSpec(memory_space=pltpu.HBM)
    vmem = pl.BlockSpec(memory_space=pltpu.VMEM)
    stream = jax.ShapeDtypeStruct((rows, width), BF)
    filt = jax.ShapeDtypeStruct((C, N), F32)
    half = jax.ShapeDtypeStruct((C, N // 2), F32)
    tap_rows = jax.ShapeDtypeStruct((TAPS, rows), F32)
    operands = (query_gate, key_gate, value_in, cotangent, long_filter, short_taps.T, table)
    outs = pl.pallas_call(
        main_kernel,
        out_shape=(stream, stream, stream, half, half, tap_rows),
        in_specs=[hbm] * len(operands),
        out_specs=(vmem,) * 6,
        scratch_shapes=[pltpu.VMEM((S, C, W), BF)] * 8
        + [pltpu.VMEM((8, W), F32)] * 4
        + [
            pltpu.VMEM((8, 2 * W), F32),
            pltpu.VMEM((PLANE, 8, 2 * W), F32),
            pltpu.VMEM((8, 2 * W), F32),
            pltpu.VMEM((HI, 8, 2 * W), F32),
            pltpu.VMEM((S * C, W), F32),
            pltpu.VMEM((S * C, W), F32),
            pltpu.VMEM((S * C, W), F32),
            pltpu.VMEM((TAPS, S * C, W), F32),
            pltpu.VMEM((S * C, 2 * W), F32),
            pltpu.VMEM((S * C, 2 * W), F32),
            pltpu.VMEM((S * C, 2 * W), F32),
        ]
        + [pltpu.VMEM(x.shape, x.dtype) for x in operands]
        + [pltpu.VMEM((2, S, W), F32)]
        + [
            pltpu.SemaphoreType.DMA((SEMAPHORES,)),
            pltpu.SemaphoreType.DMA((SEMAPHORES,)),
            pltpu.SemaphoreType.DMA((len(operands),)),
        ],
        compiler_params=pltpu.CompilerParams(
            collective_id=0, has_side_effects=True, vmem_limit_bytes=VMEM_BYTES
        ),
        name="exchange",
    )(*operands)
    *streams, tap_sums = pl.pallas_call(
        write_kernel,
        out_shape=(stream, stream, stream, filt, tap_rows),
        in_specs=[vmem] * 6,
        out_specs=(hbm,) * 5,
        scratch_shapes=[pltpu.SemaphoreType.DMA((6,))],
        compiler_params=pltpu.CompilerParams(vmem_limit_bytes=WRITE_BYTES),
        name="write",
    )(*outs)
    return (*streams, tap_sums.T)


def solution(mesh):
    spec = P("chan", "seq")
    owned = P(("chan", "seq"), None)
    taps = P("chan", None)
    return jax.shard_map(
        on_device,
        mesh=mesh,
        in_specs=(spec, spec, spec, spec, owned, taps),
        out_specs=(spec, spec, spec, owned, taps),
        check_vma=False,
    )
```
